256 devices in a mesh: samp: 64 (over z_hi, x, y), cls: 4 (over z_lo, core).
Axes of the slice: x: 4, y: 4, z: 8 (z_hi: 4, z_lo: 2; z = z_hi * 2 + z_lo), core: 2. Of those that a mesh axis runs over, the one named last changes fastest.
Arguments:
- samples: bfloat16 [8192, 32768], P('samp'), may hold values from -0.09375 to 0.09375
- labels: int32 [8192], P('samp'), may hold values from 0 to 511
- weight: bfloat16 [32768, 512], P('samp', 'cls'), may hold values from -6 to 6
- dual: float32 [8192, 512], P('samp', 'cls'), may hold values from 0 to 1
- block_inverse: float32 [512, 16, 16], P('samp'), may hold values from -0.4 to 1.2, as said below
Outputs:
- new_weight: float32 [32768, 512], P('samp', 'cls')
- new_dual: float32 [8192, 512], P('samp', 'cls')
- class_gap: float32 [512], P('cls')
- top_margin: float32 [8192], P('samp')
The draws below stay inside these ranges and needn't reach their ends.
Inputs may be any that keep to these rules, and one draw needn't show every extreme that they name: `block_inverse`: each [16, 16] matrix has a positive diagonal.
All inputs are finite; a program needn't handle non-finite values.
Results may differ from the reference program's by a relative error of at most 0.00045.
Values may be sent and summed in bfloat16 or wider, within the bound.
No kernel may reach another device: no remote copies, remote signals or barrier semaphores. Data moves between devices by JAX's collectives and lax.ppermute only.
A program may use at most 128 MiB of HBM per device.

```python
import jax
import jax.numpy as jnp
from jax import lax

FEATURES = 32768
CLASSES = 512
ROWS_DEV = 128
BLOCK = 16
PASSES = 2
SAMPLES = 8192
N_SAMP = 64


def draw_block_inverse(key, part):
    first, second = jax.random.split(jax.random.fold_in(key, 11))
    shape = (SAMPLES // BLOCK, BLOCK, BLOCK)
    spread = jnp.clip(jax.random.normal(second, shape, jnp.float32) * 0.08, -0.4, 0.4)
    diagonal = jax.random.uniform(first, (SAMPLES // BLOCK, BLOCK), jnp.float32, 0.6, 1.2)
    identity = jnp.eye(BLOCK, dtype=jnp.float32)
    return spread * (1.0 - identity) + diagonal[:, :, None] * identity


def with_ends(entries, rng, least, largest):
    index_at = [jax.random.randint(jax.random.fold_in(rng, axis), (), 0, length) for axis, length in enumerate(entries.shape)]
    widest = entries.shape.index(max(entries.shape))
    beside = index_at[:widest] + [(index_at[widest] + 1) % entries.shape[widest]] + index_at[widest + 1:]
    return entries.at[tuple(index_at)].set(least).at[tuple(beside)].set(largest)


def raised(entries, stream_key, source, target, blocks, factor):
    owner, partner = [(jnp.arange(entries.shape[axis_at]) // (entries.shape[axis_at] // blocks)).reshape([-1 if axis == axis_at else 1 for axis in range(entries.ndim)]) for axis_at in (source, target)]
    chosen = jax.random.permutation(stream_key, blocks)[partner]
    strong = (owner == chosen) | (owner == (partner + blocks // 2) % blocks)
    return jnp.where(strong, factor * entries, entries)


def block_scale(rng, shape, pieces, least, largest):
    def one(dim, parts):
        draws = jax.random.uniform(jax.random.fold_in(jax.random.fold_in(rng, 6), dim), (parts,), jnp.float32, least / len(pieces), largest / len(pieces))
        return jnp.repeat(jnp.exp(draws), shape[dim] // parts).reshape((-1,) + (1,) * (len(shape) - dim - 1))

    level = one(*pieces[0])
    for cut in pieces[1:]:
        level = level * one(*cut)
    return level


def noise(own_key, shape, scale, bound, cuts=(), held_as=jnp.bfloat16):
    gain = block_scale(own_key, shape, cuts, -0.22, 0.18) if cuts else 1.0
    result = jax.random.normal(own_key, shape, jnp.float32) * scale * gain
    return jnp.minimum(jnp.maximum(result, -bound), bound).astype(held_as)


def gaussian_with(stream_key, shape, width, reach, cuts, heavy, kind=jnp.bfloat16):
    values = width * jax.random.normal(stream_key, shape, jnp.float32)
    if cuts:
        values = values * block_scale(stream_key, shape, cuts, -0.22, 0.18)
    return jnp.clip(raised(values, jax.random.fold_in(stream_key, 3), *heavy), -reach, reach).astype(kind)


def setup_inputs(seed: int = 0) -> dict:
    key_of = jax.random.split(jax.random.key(seed), 6)
    samples = gaussian_with(key_of[0], (SAMPLES, FEATURES), (FEATURES ** -0.5), 0.09375, ((0, 64),), (0, 1, 64, 4.0))
    labels = with_ends(jax.random.randint(key_of[1], (SAMPLES,), 0, CLASSES), jax.random.fold_in(key_of[1], 1), 0, CLASSES - 1).astype(jnp.int32)
    weight = noise(key_of[2], (FEATURES, CLASSES), 1.0, 6.0, ((0, 64), (1, 4)))
    dual = jnp.clip(1.0 * jax.random.uniform(key_of[3], (SAMPLES, CLASSES), jnp.float32) ** block_scale(key_of[3], (SAMPLES, CLASSES), ((0, 64), (1, 4)), -0.2, 0.2), 0.0, 1.0)
    block_inverse = draw_block_inverse(jax.random.fold_in(key_of[5], 71), 0)
    return {"samples": samples, "labels": labels, "weight": weight, "dual": dual, "block_inverse": block_inverse}


coupling = 0.5


def dual_passes(gram, start, sign, dual, inverse):
    rows = start.shape[0]
    blocks = rows // BLOCK

    def visit(turn, carry):
        alpha, change = carry
        index = (turn % blocks).astype(jnp.int32)
        low = (index * BLOCK).astype(jnp.int32)
        gram_rows = lax.dynamic_slice_in_dim(gram, low, BLOCK, 0)
        start_rows = lax.dynamic_slice_in_dim(start, low, BLOCK, 0)
        sign_rows = lax.dynamic_slice_in_dim(sign, low, BLOCK, 0)
        dual_rows = lax.dynamic_slice_in_dim(dual, low, BLOCK, 0)
        alpha_rows = lax.dynamic_slice_in_dim(alpha, low, BLOCK, 0)
        matrix = lax.dynamic_index_in_dim(inverse, index, 0, keepdims=False)
        margin = start_rows + coupling * jnp.dot(gram_rows, change, precision=lax.Precision.HIGHEST)
        ascent = jnp.dot(matrix, 1.0 - sign_rows * margin, precision=lax.Precision.HIGHEST)
        alpha_rows = jnp.clip(alpha_rows + ascent, 0.0, 1.0)
        change_rows = sign_rows * (alpha_rows - dual_rows)
        alpha = lax.dynamic_update_slice_in_dim(alpha, alpha_rows, low, 0)
        change = lax.dynamic_update_slice_in_dim(change, change_rows, low, 0)
        return alpha, change

    alpha, change = lax.fori_loop(0, PASSES * blocks, visit, (dual, jnp.zeros_like(dual)))
    margin = start + coupling * jnp.dot(gram, change, precision=lax.Precision.HIGHEST)
    return alpha, margin, change


def reference(samples, labels, weight, dual, block_inverse):
    class_ids = jnp.arange(CLASSES, dtype=jnp.int32)
    sign = jnp.where(labels[:, None] == class_ids[None, :], 1.0, -1.0).astype(jnp.float32)
    start = jnp.dot(samples, weight, preferred_element_type=jnp.float32)
    scaled = sign * start
    terms = jnp.maximum(0.0, 1.0 - scaled) + dual * (scaled - 1.0)
    class_gap = jnp.sum(terms, axis=0) / SAMPLES

    blocks = ROWS_DEV // BLOCK

    def group(inputs):
        rows_x, rows_start, rows_sign, rows_dual, rows_inv = inputs
        gram = lax.dot_general(rows_x, rows_x, (((1,), (1,)), ((), ())), preferred_element_type=jnp.float32)
        return dual_passes(gram, rows_start, rows_sign, rows_dual, rows_inv)

    alpha, margin, change = lax.map(group, (
        samples.reshape(N_SAMP, ROWS_DEV, FEATURES),
        start.reshape(N_SAMP, ROWS_DEV, CLASSES),
        sign.reshape(N_SAMP, ROWS_DEV, CLASSES),
        dual.reshape(N_SAMP, ROWS_DEV, CLASSES),
        block_inverse.reshape(N_SAMP, blocks, BLOCK, BLOCK)))
    new_dual = alpha.reshape(SAMPLES, CLASSES)
    top_margin = jnp.max(margin.reshape(SAMPLES, CLASSES), axis=1)
    steps = change.reshape(SAMPLES, CLASSES).astype(jnp.bfloat16)
    delta = lax.dot_general(samples, steps, (((0,), (0,)), ((), ())), preferred_element_type=jnp.float32)
    new_weight = weight.astype(jnp.float32) + coupling * delta
    return new_weight, new_dual, class_gap, top_margin
```

```python
import functools

import jax
import jax.numpy as jnp
from jax import lax
from jax.experimental import pallas as pl
from jax.experimental.pallas import tpu as pltpu
from jax.sharding import Mesh, PartitionSpec as P


BLOCK = 16
PASSES = 2
COUPLING = 0.5

ZH, X, Y, ZL, CORE = "zh", "x", "y", "zl", "core"
PLANE = (X, Y)
SAMP = (ZH, X, Y)
CLS = (ZL, CORE)
GAP_ROWS = 8
ORDER = (0, 2, 1, 3)
F32, BF16 = jnp.float32, jnp.bfloat16
SMALL = pltpu.CompilerParams(vmem_limit_bytes=16 * 2**20)


def shifted(value, axis, by):
    size = lax.axis_size(axis)
    return lax.ppermute(value, axis, [(i, (i + by) % size) for i in range(size)])


def pack_kernel(where, rows_ref, out_ref):
    width = out_ref.shape[2]
    for place in range(out_ref.shape[0]):
        out_ref[place] = rows_ref[:, place * width:(place + 1) * width]


def pack(samples, where, planes, members, quarters):
    rows, features = samples.shape
    part = rows // quarters
    width = features // (planes * members)
    return pl.pallas_call(
        pack_kernel,
        grid_spec=pltpu.PrefetchScalarGridSpec(
            num_scalar_prefetch=1,
            grid=(planes,),
            in_specs=[pl.BlockSpec((part, features // planes), lambda k, where: (where[0], lax.rem(where[1] + (planes - k), planes)))],
            out_specs=pl.BlockSpec((members, part, width), lambda k, where: (0, 0, k)),
        ),
        out_shape=jax.ShapeDtypeStruct((members, part, planes * width), samples.dtype),
        name="pack",
    )(where, samples)


def exact_dot(a, b):
    return jnp.dot(a, b, precision=lax.Precision.HIGHEST, preferred_element_type=F32)


def three_pieces(value):
    first = value.astype(BF16)
    rest = value - first.astype(F32)
    second = rest.astype(BF16)
    third = (rest - second.astype(F32)).astype(BF16)
    return first, second, third


def passes_kernel(where, start_ref, gram_ref, labels_ref, dual_ref, inverse_ref,
                  alpha_ref, steps_ref, top_ref, sign_ref, margin_ref, change_ref):
    rows, width = start_ref.shape
    class_ids = where[0] * width + lax.broadcasted_iota(jnp.int32, (rows, width), 1)
    sign = jnp.where(labels_ref[...] == class_ids, 1.0, -1.0).astype(F32)
    sign_ref[...] = sign
    start = start_ref[...]
    margin_ref[...] = start
    alpha_ref[...] = dual_ref[...]
    change_ref[...] = jnp.zeros((rows, width), F32)
    scaled = sign * start
    gap = jnp.sum(jnp.maximum(0.0, 1.0 - scaled) + dual_ref[...] * (scaled - 1.0), axis=0, keepdims=True)
    for turn in range(PASSES * (rows // BLOCK)):
        b = turn % (rows // BLOCK)
        at = slice(b * BLOCK, (b + 1) * BLOCK)
        signs = sign_ref[at]
        ascent = exact_dot(inverse_ref[b], 1.0 - signs * margin_ref[at])
        alpha = jnp.clip(alpha_ref[at] + ascent, 0.0, 1.0)
        change = signs * (alpha - dual_ref[at])
        moved = change - change_ref[at]
        alpha_ref[at] = alpha
        change_ref[at] = change
        margin_ref[...] += COUPLING * exact_dot(gram_ref[:, at], moved)
    top_ref[...] = jnp.max(margin_ref[...], axis=1, keepdims=True)
    payload = change_ref[...].astype(BF16)
    tail = tail_of(gap)
    for place in range(steps_ref.shape[0]):
        steps_ref[place, :rows] = payload
        steps_ref[place, rows:] = tail


def passes(where, start, gram, labels, dual, inverse, members):
    rows, width = start.shape
    whole = pl.BlockSpec(memory_space=pltpu.VMEM)
    return pl.pallas_call(
        passes_kernel,
        in_specs=[pl.BlockSpec(memory_space=pltpu.SMEM)] + [whole] * 5,
        out_specs=[whole] * 3,
        out_shape=[
            jax.ShapeDtypeStruct((rows, width), F32),
            jax.ShapeDtypeStruct((members, rows + GAP_ROWS, width), BF16),
            jax.ShapeDtypeStruct((rows, 1), F32),
        ],
        scratch_shapes=[pltpu.VMEM((rows, width), F32)] * 3,
        compiler_params=SMALL,
        name="passes",
    )(where, start, gram, labels, dual, inverse)


def tail_of(gap):
    first, second, third = three_pieces(gap)
    row = lax.broadcasted_iota(jnp.int32, (GAP_ROWS, gap.shape[1]), 0)
    zero = jnp.zeros((GAP_ROWS, gap.shape[1]), F32)
    return jnp.where(row == 0, first.astype(F32), jnp.where(row == 1, second.astype(F32), jnp.where(row == 2, third.astype(F32), zero))).astype(BF16)


def from_tail(tail):
    tail = tail.astype(F32)
    return (tail[0:1] + tail[1:2]) + tail[2:3]


def product(turned_ref, quarter_refs):
    total, d, low = None, 0, 0
    for ref in quarter_refs:
        high = low + ref.shape[0]
        term = jnp.dot(turned_ref[d, :, low:high], ref[...], preferred_element_type=F32)
        total = term if total is None else total + term
        d, low = (d + 1, 0) if high == turned_ref.shape[2] else (d, high)
    return total.T


def first_delta_kernel(where, *refs):
    *held, steps_ref, sent_ref, turned_ref, gap_ref = refs
    members, _, width = steps_ref.shape
    quarters = turned_ref.shape[0]
    part = turned_ref.shape[2] // members
    rows = quarters * part
    for d in range(quarters):
        low = pl.multiple_of(lax.bitwise_xor(where[0], d) * part, part)
        picked = jnp.concatenate([steps_ref[g, pl.ds(low, part), :] for g in range(members)], axis=0)
        turned_ref[d] = picked.astype(F32).T.astype(BF16)
    gap = jnp.zeros((1, width), F32)
    for g in range(members):
        gap += from_tail(steps_ref[g, rows:, :])
    gap_ref[...] = gap
    delta = product(turned_ref, held)
    depth = delta.shape[0]
    sent_ref[:depth] = delta.astype(BF16)
    sent_ref[depth:] = tail_of(gap)


def next_delta_kernel(where, *refs):
    *held, turned_ref, gap_ref, sent_ref = refs
    delta = product(turned_ref, held)
    depth = delta.shape[0]
    sent_ref[:depth] = delta.astype(BF16)
    sent_ref[depth:] = tail_of(gap_ref[...])


def own_delta_kernel(where, *refs):
    *held, turned_ref, sum_ref = refs
    sum_ref[...] = product(turned_ref, held)


def finish_kernel(count, weight_ref, own_ref, gap_ref, *refs):
    *came, new_ref, class_gap_ref = refs
    depth = own_ref.shape[0]
    total, gap = own_ref[...], gap_ref[...]
    for ref in came:
        total += ref[:depth].astype(F32)
        gap += from_tail(ref[depth:])
    new_ref[...] = weight_ref[...].astype(F32) + COUPLING * total
    class_gap_ref[...] = gap / count


def finish(weight, own, gap, came, count):
    depth, width = weight.shape
    whole = pl.BlockSpec(memory_space=pltpu.VMEM)
    return pl.pallas_call(
        functools.partial(finish_kernel, count),
        in_specs=[whole] * (3 + len(came)),
        out_specs=[whole] * 2,
        out_shape=[jax.ShapeDtypeStruct((depth, width), F32), jax.ShapeDtypeStruct((1, width), F32)],
        compiler_params=SMALL,
        name="finish",
    )(weight, own, gap, *came)


def column_specs(quarters, planes, k):
    return [pl.BlockSpec((held.shape[0], held.shape[1] // planes), lambda *_: (0, k)) for held in quarters]


def whole_spec(shape):
    return pl.BlockSpec(shape, lambda *_: (0,) * len(shape))


def first_delta(where, quarters, steps, planes, k):
    total, features = quarters[0].shape
    width = steps.shape[2]
    shapes = [
        jax.ShapeDtypeStruct((features // planes + GAP_ROWS, width), BF16),
        jax.ShapeDtypeStruct((len(ORDER), width, total), BF16),
        jax.ShapeDtypeStruct((1, width), F32),
    ]
    return pl.pallas_call(
        first_delta_kernel,
        grid_spec=pltpu.PrefetchScalarGridSpec(
            num_scalar_prefetch=1,
            grid=(1,),
            in_specs=column_specs(quarters, planes, k) + [whole_spec(steps.shape)],
            out_specs=[whole_spec(shape.shape) for shape in shapes],
        ),
        out_shape=shapes,
        compiler_params=SMALL,
        name="delta_first",
    )(where, *quarters, steps)


def next_delta(where, quarters, turned, gap, planes, k):
    shape = jax.ShapeDtypeStruct((quarters[0].shape[1] // planes + GAP_ROWS, gap.shape[1]), BF16)
    return pl.pallas_call(
        next_delta_kernel,
        grid_spec=pltpu.PrefetchScalarGridSpec(
            num_scalar_prefetch=1,
            grid=(1,),
            in_specs=column_specs(quarters, planes, k) + [whole_spec(turned.shape), whole_spec(gap.shape)],
            out_specs=whole_spec(shape.shape),
        ),
        out_shape=shape,
        compiler_params=SMALL,
        name="delta_next",
    )(where, *quarters, turned, gap)


def own_delta(where, quarters, turned, planes):
    shape = jax.ShapeDtypeStruct((quarters[0].shape[1] // planes, turned.shape[1]), F32)
    return pl.pallas_call(
        own_delta_kernel,
        grid_spec=pltpu.PrefetchScalarGridSpec(
            num_scalar_prefetch=1,
            grid=(1,),
            in_specs=column_specs(quarters, planes, 0) + [whole_spec(turned.shape)],
            out_specs=whole_spec(shape.shape),
        ),
        out_shape=shape,
        compiler_params=SMALL,
        name="delta_own",
    )(where, *quarters, turned)


def gathered_kernel(where, parts_ref, out_ref):
    members = parts_ref.shape[0]
    width = out_ref.shape[2]
    total = parts_ref[0]
    for g in range(1, members):
        total += parts_ref[g]
    for i, d in enumerate(ORDER):
        out_ref[lax.bitwise_xor(where[0], d)] = total[:, i * width:(i + 1) * width]


def gathered(where, parts):
    _, part, total = parts.shape
    return pl.pallas_call(
        gathered_kernel,
        in_specs=[pl.BlockSpec(memory_space=pltpu.SMEM), pl.BlockSpec(memory_space=pltpu.VMEM)],
        out_specs=pl.BlockSpec(memory_space=pltpu.VMEM),
        out_shape=jax.ShapeDtypeStruct((len(ORDER), part, total // len(ORDER)), F32),
        compiler_params=SMALL,
        name="gathered",
    )(where, parts)


def round_of_ascent(samples, labels, weight, dual, inverse):
    rows = samples.shape[0]
    depth, width = weight.shape
    planes = lax.axis_size(ZH)
    members = lax.axis_size(X) * lax.axis_size(Y)
    quarters = lax.axis_size(ZL) * lax.axis_size(CORE)
    part = rows // quarters
    mine = lax.axis_index(CLS).astype(jnp.int32)
    where = jnp.stack([mine, lax.axis_index(ZH).astype(jnp.int32)])

    packed = pack(samples, where, planes, members, quarters)
    quarter = lax.all_to_all(packed, PLANE, split_axis=0, concat_axis=0, tiled=True)
    near = [weight]
    for k in range(1, planes):
        near.append(shifted(weight, ZH, k))
    pairs = [jnp.concatenate([piece, shifted(piece, ZL, 1)], axis=1) for piece in near]
    by_pair = jnp.concatenate(pairs, axis=0)
    by_all = jnp.concatenate([by_pair, shifted(by_pair, CORE, 1)], axis=1)
    gram = lax.dot_general(samples, samples, (((1,), (1,)), ((), ())), preferred_element_type=F32)

    flat = quarter.reshape(members * part, planes * depth)
    half = members * part // 2
    beside_a = shifted(flat[:half], ZL, 1)
    partial = jnp.dot(flat, by_all, preferred_element_type=F32)
    partial = lax.all_to_all(partial.reshape(members, part, quarters * width), PLANE, split_axis=0, concat_axis=0, tiled=True)
    across = shifted(flat, CORE, 1)
    diagonal_a = shifted(beside_a, CORE, 1)
    pieces = gathered(where, partial)
    start = lax.all_to_all(pieces, CLS, split_axis=0, concat_axis=0, tiled=True).reshape(rows, width)
    beside_b = shifted(flat[half:], ZL, 1)

    alpha, steps, top = passes(where, start, gram, labels[:, None], dual, inverse, members)
    steps = lax.all_to_all(steps, PLANE, split_axis=0, concat_axis=0, tiled=True)
    diagonal_b = shifted(beside_b, CORE, 1)

    top = top[:, 0]
    other = shifted(top, CORE, 1)
    top = jnp.maximum(top, other)
    other = shifted(top, ZL, 1)
    top = jnp.maximum(top, other)

    held = [flat, across, beside_a, beside_b, diagonal_a, diagonal_b]
    far = planes // 2
    sent, turned, gap = first_delta(where, held, steps, planes, far)
    came = [shifted(sent, ZH, planes - far)]
    for k in range(1, planes):
        if k != far:
            sent = next_delta(where, held, turned, gap, planes, k)
            came.append(shifted(sent, ZH, planes - k))
    own = own_delta(where, held, turned, planes)
    new_weight, gap = finish(weight, own, gap, came, rows * planes * members)
    return new_weight, alpha, gap[0], top


def solution(mesh):
    fine = Mesh(mesh.devices.reshape(4, 4, 4, 2, 2), (ZH, X, Y, ZL, CORE))
    return jax.shard_map(
        round_of_ascent,
        mesh=fine,
        in_specs=(P(SAMP, None), P(SAMP), P(SAMP, CLS), P(SAMP, CLS), P(SAMP, None, None)),
        out_specs=(P(SAMP, CLS), P(SAMP, CLS), P(CLS), P(SAMP)),
        check_vma=False,
    )
```

```python
import functools

import jax
import jax.numpy as jnp
from jax import lax
from jax.experimental import pallas as pl
from jax.experimental.pallas import tpu as pltpu
from jax.sharding import Mesh, PartitionSpec as P


BLOCK = 16
PASSES = 2
COUPLING = 0.5

ZH, X, Y, ZL, CORE = "zh", "x", "y", "zl", "core"
PLANE = (X, Y)
SAMP = (ZH, X, Y)
CLS = (ZL, CORE)
GAP_ROWS = 8
EARLY = 10
ORDER = (0, 2, 1, 3)
F32, BF16 = jnp.float32, jnp.bfloat16
IN_VMEM = pl.BlockSpec(memory_space=pltpu.VMEM)
IN_SMEM = pl.BlockSpec(memory_space=pltpu.SMEM)
IN_HBM = pl.BlockSpec(memory_space=pltpu.HBM)
LEFT = (0, 0, 1, 1, 0, 2)
RIGHT = (0, 1, 0, 1, 2, 0)
SMALL = pltpu.CompilerParams(vmem_limit_bytes=16 * 2**20)
FULL = pltpu.CompilerParams(vmem_limit_bytes=60 * 1024 * 1024)


def shifted(value, axis, by):
    size = lax.axis_size(axis)
    return lax.ppermute(value, axis, [(i, (i + by) % size) for i in range(size)])


def pack_kernel(where, rows_hbm, out_hbm, held_ref, in_sems, out_sems):
    members, part, total = out_hbm.shape
    planes = in_sems.shape[0]
    width = total // planes
    span = members * width
    row = pl.multiple_of(where[0] * part, part)
    loads = []
    for k in range(planes):
        low = pl.multiple_of(lax.rem(where[1] + (planes - k), planes) * span, span)
        loads.append(pltpu.make_async_copy(rows_hbm.at[pl.ds(row, part), pl.ds(low, span)], held_ref.at[k], in_sems.at[k]))
    for load in loads:
        load.start()
    stores = []
    for k in range(planes):
        loads[k].wait()
        for place in range(members):
            store = pltpu.make_async_copy(
                held_ref.at[k, :, pl.ds(place * width, width)],
                out_hbm.at[place, :, pl.ds(k * width, width)],
                out_sems.at[k * members + place],
            )
            store.start()
            stores.append(store)
    for store in stores:
        store.wait()


def pack(samples, where, planes, members, quarters):
    rows, features = samples.shape
    part = rows // quarters
    return pl.pallas_call(
        pack_kernel,
        in_specs=[IN_SMEM, IN_HBM],
        out_specs=IN_HBM,
        out_shape=jax.ShapeDtypeStruct((members, part, features // members), samples.dtype),
        scratch_shapes=[
            pltpu.VMEM((planes, part, features // planes), samples.dtype),
            pltpu.SemaphoreType.DMA((planes,)),
            pltpu.SemaphoreType.DMA((planes * members,)),
        ],
        compiler_params=FULL,
        name="pack",
    )(where, samples)


def three_pieces(value):
    first = value.astype(BF16)
    rest = value - first.astype(F32)
    second = rest.astype(BF16)
    third = (rest - second.astype(F32)).astype(BF16)
    return first, second, third


def prepare_kernel(gram_ref, inverse_ref, expanded_ref, wide_ref):
    rows = gram_ref.shape[0]
    _, size, _ = inverse_ref.shape
    lanes = expanded_ref.shape[3]
    b = pl.program_id(0)
    low = pl.multiple_of(b * size, size)
    high = pl.multiple_of(lax.rem(b + 1, pl.num_programs(0)) * size, size)
    spot = lax.broadcasted_iota(jnp.int32, (rows, size), 0) == low + lax.broadcasted_iota(jnp.int32, (rows, size), 1)
    picks = jnp.where(spot, 1.0, 0.0).astype(BF16)
    sides = [jnp.dot(piece, picks, preferred_element_type=F32) for piece in three_pieces(COUPLING * gram_ref[...])]
    exact = jnp.dot(gram_ref[pl.ds(high, size)], jnp.where(spot, 1.0, 0.0), precision=lax.Precision.HIGHEST, preferred_element_type=F32)
    for k in range(size):
        expanded_ref[0, k] = jnp.broadcast_to(inverse_ref[0, :, k:k + 1], (size, lanes))
        expanded_ref[0, size + k] = COUPLING * jnp.broadcast_to(exact[:, k:k + 1], (size, lanes))
    wide_ref[0] = jnp.concatenate([sides[p].astype(BF16) for p in LEFT], axis=1)


def prepare(gram, inverse, lanes):
    rows = gram.shape[0]
    blocks, size, _ = inverse.shape
    return pl.pallas_call(
        prepare_kernel,
        grid=(blocks,),
        in_specs=[pl.BlockSpec((rows, rows), lambda b: (0, 0)), pl.BlockSpec((1, size, size), lambda b: (b, 0, 0))],
        out_specs=[
            pl.BlockSpec((1, 2 * size, size, lanes), lambda b: (b, 0, 0, 0)),
            pl.BlockSpec((1, rows, len(LEFT) * size), lambda b: (b, 0, 0)),
        ],
        out_shape=[
            jax.ShapeDtypeStruct((blocks, 2 * size, size, lanes), F32),
            jax.ShapeDtypeStruct((blocks, rows, len(LEFT) * size), BF16),
        ],
        compiler_params=FULL,
        name="prepare",
    )(gram, inverse)


def rows_product(expanded, value):
    size = value.shape[0]
    sums = []
    for k in range(size):
        term = expanded[k] * jnp.broadcast_to(value[k:k + 1], value.shape)
        if k < 4:
            sums.append(term)
        else:
            sums[k % 4] += term
    return (sums[0] + sums[1]) + (sums[2] + sums[3])


def passes_kernel(where, start_hbm, labels_hbm, dual_hbm, expanded_hbm, wide_hbm, alpha_hbm, steps_hbm, top_hbm,
                  margin_ref, labels_ref, dual_ref, expanded_ref, wide_ref, alpha_ref, start_ref, sign_ref, change_ref, payload_ref, top_ref, sems):
    rows, width = margin_ref.shape
    blocks = rows // BLOCK
    copies = [
        pltpu.make_async_copy(start_hbm, start_ref, sems.at[0]),
        pltpu.make_async_copy(labels_hbm, labels_ref, sems.at[1]),
        pltpu.make_async_copy(dual_hbm, dual_ref, sems.at[2]),
    ]
    parts = [
        [pltpu.make_async_copy(expanded_hbm.at[b], expanded_ref.at[b], sems.at[3 + b]),
         pltpu.make_async_copy(wide_hbm.at[b], wide_ref.at[b], sems.at[3 + blocks + b])]
        for b in range(blocks)
    ]
    for copy in copies + [part for pair in parts for part in pair]:
        copy.start()
    change_ref[...] = jnp.zeros((rows, width), F32)
    for copy in copies:
        copy.wait()
    class_ids = where[0] * width + lax.broadcasted_iota(jnp.int32, (rows, width), 1)
    sign_ref[...] = jnp.where(labels_ref[...] == class_ids, 1.0, -1.0).astype(F32)
    margin_ref[...] = start_ref[...]
    alpha_ref[...] = dual_ref[...]
    margin = start_ref[:BLOCK]
    for turn in range(PASSES * blocks):
        b = turn % blocks
        at = slice(b * BLOCK, (b + 1) * BLOCK)
        n = (b + 1) % blocks
        if turn < blocks:
            for copy in parts[b]:
                copy.wait()
        signs = sign_ref[at]
        ascent = rows_product(expanded_ref[b, :BLOCK], 1.0 - signs * margin)
        alpha = jnp.clip(alpha_ref[at] + ascent, 0.0, 1.0)
        change = signs * (alpha - dual_ref[at])
        moved = change - change_ref[at]
        alpha_ref[at] = alpha
        change_ref[at] = change
        margin = margin_ref[n * BLOCK:(n + 1) * BLOCK] + rows_product(expanded_ref[b, BLOCK:], moved)
        pieces = three_pieces(moved)
        tall = jnp.concatenate([pieces[p] for p in RIGHT], axis=0)
        margin_ref[...] += jnp.dot(wide_ref[b], tall, preferred_element_type=F32)
    scaled = sign_ref[...] * start_ref[...]
    gap = jnp.sum(jnp.maximum(0.0, 1.0 - scaled) + dual_ref[...] * (scaled - 1.0), axis=0, keepdims=True)
    payload_ref[:rows] = change_ref[...].astype(BF16)
    payload_ref[rows:] = tail_of(gap)
    outs = [pltpu.make_async_copy(payload_ref, steps_hbm.at[place], sems.at[place]) for place in range(steps_hbm.shape[0])]
    for copy in outs:
        copy.start()
    top_ref[...] = jnp.max(margin_ref[...].T, axis=0, keepdims=True)
    after = steps_hbm.shape[0]
    outs += [pltpu.make_async_copy(alpha_ref, alpha_hbm, sems.at[after]), pltpu.make_async_copy(top_ref, top_hbm, sems.at[after + 1])]
    for copy in outs[after:]:
        copy.start()
    for copy in outs:
        copy.wait()


def passes(where, start, labels, dual, ready, members):
    rows, width = start.shape
    square = pltpu.VMEM((rows, width), F32)
    return pl.pallas_call(
        passes_kernel,
        in_specs=[IN_SMEM] + [IN_HBM] * 5,
        out_specs=[IN_HBM] * 3,
        out_shape=[
            jax.ShapeDtypeStruct((rows, width), F32),
            jax.ShapeDtypeStruct((members, rows + GAP_ROWS, width), BF16),
            jax.ShapeDtypeStruct((1, rows), F32),
        ],
        scratch_shapes=[
            square,
            pltpu.VMEM(labels.shape, labels.dtype),
            square,
            pltpu.VMEM(ready[0].shape, ready[0].dtype),
            pltpu.VMEM(ready[1].shape, ready[1].dtype),
            square,
            square,
            square,
            square,
            pltpu.VMEM((rows + GAP_ROWS, width), BF16),
            pltpu.VMEM((1, rows), F32),
            pltpu.SemaphoreType.DMA((3 + 2 * (rows // BLOCK),)),
        ],
        compiler_params=FULL,
        name="passes",
    )(where, start, labels, dual, *ready)


def tail_of(gap):
    first, second, third = three_pieces(gap)
    row = lax.broadcasted_iota(jnp.int32, (GAP_ROWS, gap.shape[1]), 0)
    zero = jnp.zeros((GAP_ROWS, gap.shape[1]), F32)
    return jnp.where(row == 0, first.astype(F32), jnp.where(row == 1, second.astype(F32), jnp.where(row == 2, third.astype(F32), zero))).astype(BF16)


def from_tail(tail):
    tail = tail.astype(F32)
    return (tail[0:1] + tail[1:2]) + tail[2:3]


def fetches(held_refs, block_ref, sems, k):
    depth = block_ref.shape[1]
    copies, low = [], 0
    for i, ref in enumerate(held_refs):
        rows = ref.shape[0]
        copies.append(pltpu.make_async_copy(ref.at[:, pl.ds(k * depth, depth)], block_ref.at[pl.ds(low, rows)], sems.at[i]))
        low += rows
    for copy in copies:
        copy.start()
    return copies


def lanes_of(rows):
    return -(-rows // 128) * 128


def product(turned_ref, block_ref, copies, heights):
    total, low, at = None, 0, 0
    for copy, rows in zip(copies, heights):
        copy.wait()
        term = jnp.dot(turned_ref[:, at:at + rows], block_ref[low:low + rows], preferred_element_type=F32)
        total = term if total is None else total + term
        low += rows
        at += lanes_of(rows)
    return total.T


def first_delta_kernel(k, where, *refs):
    *held, steps_ref, sent_ref, turned_ref, gap_ref, block_ref, sems = refs
    copies = fetches(held, block_ref, sems, k)
    members, tall, width = steps_ref.shape
    rows = tall - GAP_ROWS
    part = rows // len(ORDER)
    d, first, at = 0, 0, 0
    for ref in held:
        count = ref.shape[0] // part
        low = pl.multiple_of(lax.bitwise_xor(where[0], d) * part, part)
        picked = jnp.concatenate([steps_ref[g, pl.ds(low, part), :] for g in range(first, first + count)], axis=0)
        turned_ref[:, at:at + count * part] = picked.astype(F32).T.astype(BF16)
        at += lanes_of(count * part)
        d, first = (d + 1, 0) if first + count == members else (d, first + count)
    gap = jnp.zeros((1, width), F32)
    for g in range(members):
        gap += from_tail(steps_ref[g, rows:, :])
    gap_ref[...] = gap
    delta = product(turned_ref, block_ref, copies, [ref.shape[0] for ref in held])
    depth = delta.shape[0]
    sent_ref[:depth] = delta.astype(BF16)
    sent_ref[depth:] = tail_of(gap)


def next_delta_kernel(k, *refs):
    *held, turned_ref, gap_ref, sent_ref, block_ref, sems = refs
    copies = fetches(held, block_ref, sems, k)
    delta = product(turned_ref, block_ref, copies, [ref.shape[0] for ref in held])
    depth = delta.shape[0]
    sent_ref[:depth] = delta.astype(BF16)
    sent_ref[depth:] = tail_of(gap_ref[...])


def own_delta_kernel(*refs):
    *held, turned_ref, sum_ref, block_ref, sems = refs
    copies = fetches(held, block_ref, sems, 0)
    sum_ref[...] = product(turned_ref, block_ref, copies, [ref.shape[0] for ref in held])


def finish_kernel(count, weight_ref, own_ref, gap_ref, *refs):
    *came, new_ref, class_gap_ref = refs
    depth = own_ref.shape[0]
    total, gap = own_ref[...], gap_ref[...]
    for ref in came:
        total += ref[:depth].astype(F32)
        gap += from_tail(ref[depth:])
    new_ref[...] = weight_ref[...].astype(F32) + COUPLING * total
    class_gap_ref[...] = gap / count


def finish(weight, own, gap, came, count):
    depth, width = weight.shape
    whole = pl.BlockSpec(memory_space=pltpu.VMEM)
    return pl.pallas_call(
        functools.partial(finish_kernel, count),
        in_specs=[whole] * (3 + len(came)),
        out_specs=[whole] * 2,
        out_shape=[jax.ShapeDtypeStruct((depth, width), F32), jax.ShapeDtypeStruct((1, width), F32)],
        compiler_params=SMALL,
        name="finish",
    )(weight, own, gap, *came)


def block_scratch(quarters, planes):
    rows = sum(held.shape[0] for held in quarters)
    return [pltpu.VMEM((rows, quarters[0].shape[1] // planes), BF16), pltpu.SemaphoreType.DMA((len(quarters),))]


def first_delta(where, quarters, steps, planes, k):
    features = quarters[0].shape[1]
    width = steps.shape[2]
    return pl.pallas_call(
        functools.partial(first_delta_kernel, k),
        in_specs=[IN_SMEM] + [IN_HBM] * len(quarters) + [IN_VMEM],
        out_specs=[IN_VMEM] * 3,
        out_shape=[
            jax.ShapeDtypeStruct((features // planes + GAP_ROWS, width), BF16),
            jax.ShapeDtypeStruct((width, sum(lanes_of(held.shape[0]) for held in quarters)), BF16),
            jax.ShapeDtypeStruct((1, width), F32),
        ],
        scratch_shapes=block_scratch(quarters, planes),
        compiler_params=SMALL,
        name="delta_first",
    )(where, *quarters, steps)


def next_delta(quarters, turned, gap, planes, k):
    return pl.pallas_call(
        functools.partial(next_delta_kernel, k),
        in_specs=[IN_HBM] * len(quarters) + [IN_VMEM] * 2,
        out_specs=IN_VMEM,
        out_shape=jax.ShapeDtypeStruct((quarters[0].shape[1] // planes + GAP_ROWS, gap.shape[1]), BF16),
        scratch_shapes=block_scratch(quarters, planes),
        compiler_params=SMALL,
        name="delta_next",
    )(*quarters, turned, gap)


def own_delta(quarters, turned, planes):
    return pl.pallas_call(
        own_delta_kernel,
        in_specs=[IN_HBM] * len(quarters) + [IN_VMEM],
        out_specs=IN_VMEM,
        out_shape=jax.ShapeDtypeStruct((quarters[0].shape[1] // planes, turned.shape[0]), F32),
        scratch_shapes=block_scratch(quarters, planes),
        compiler_params=SMALL,
        name="delta_own",
    )(*quarters, turned)


def gathered_kernel(where, parts_ref, out_ref):
    members = parts_ref.shape[0]
    width = out_ref.shape[2]
    total = parts_ref[0]
    for g in range(1, members):
        total += parts_ref[g]
    for i, d in enumerate(ORDER):
        out_ref[lax.bitwise_xor(where[0], d)] = total[:, i * width:(i + 1) * width]


def gathered(where, parts):
    _, part, total = parts.shape
    return pl.pallas_call(
        gathered_kernel,
        in_specs=[pl.BlockSpec(memory_space=pltpu.SMEM), pl.BlockSpec(memory_space=pltpu.VMEM)],
        out_specs=pl.BlockSpec(memory_space=pltpu.VMEM),
        out_shape=jax.ShapeDtypeStruct((len(ORDER), part, total // len(ORDER)), F32),
        compiler_params=FULL,
        name="gathered",
    )(where, parts)


def round_of_ascent(samples, labels, weight, dual, inverse):
    rows = samples.shape[0]
    depth, width = weight.shape
    planes = lax.axis_size(ZH)
    members = lax.axis_size(X) * lax.axis_size(Y)
    quarters = lax.axis_size(ZL) * lax.axis_size(CORE)
    part = rows // quarters
    mine = lax.axis_index(CLS).astype(jnp.int32)
    where = jnp.stack([mine, lax.axis_index(ZH).astype(jnp.int32)])

    packed = pack(samples, where, planes, members, quarters)
    quarter = lax.all_to_all(packed, PLANE, split_axis=0, concat_axis=0, tiled=True)
    near, lines = [weight], []
    for k in range(1, planes):
        near.append(shifted(weight, ZH, k))
    for k in range(planes):
        lines.append(shifted(near[k], ZL, 1))
    by_pair = jnp.concatenate([jnp.concatenate(pair, axis=1) for pair in zip(near, lines)], axis=0)
    by_all = jnp.concatenate([by_pair, shifted(by_pair, CORE, 1)], axis=1)
    gram = lax.dot_general(samples, samples, (((1,), (1,)), ((), ())), preferred_element_type=F32)

    flat = quarter.reshape(members * part, planes * depth)
    early = members * EARLY // 16 * part
    beside_a = shifted(flat[:early], ZL, 1)
    partial = jnp.dot(flat, by_all, preferred_element_type=F32)
    partial = lax.all_to_all(partial.reshape(members, part, quarters * width), PLANE, split_axis=0, concat_axis=0, tiled=True)
    across = shifted(flat, CORE, 1)
    diagonal_a = shifted(beside_a, CORE, 1)
    partial, late = lax.optimization_barrier((partial, flat))
    pieces = gathered(where, partial)
    start = lax.all_to_all(pieces, CLS, split_axis=0, concat_axis=0, tiled=True).reshape(rows, width)
    beside_b = shifted(late[early:], ZL, 1)

    ready = prepare(gram, inverse, width)
    alpha, steps, top = passes(where, start, labels[:, None], dual, ready, members)
    steps = lax.all_to_all(steps, PLANE, split_axis=0, concat_axis=0, tiled=True)
    diagonal_b = shifted(beside_b, CORE, 1)

    top = top[0]
    other = shifted(top, CORE, 1)
    top = jnp.maximum(top, other)
    other = shifted(top, ZL, 1)
    top = jnp.maximum(top, other)

    held = [flat, across, beside_a, beside_b, diagonal_a, diagonal_b]
    far = planes // 2
    sent, turned, gap = first_delta(where, held, steps, planes, far)
    came = [shifted(sent, ZH, planes - far)]
    for k in range(1, planes):
        if k != far:
            sent = next_delta(held, turned, gap, planes, k)
            came.append(shifted(sent, ZH, planes - k))
    own = own_delta(held, turned, planes)
    new_weight, gap = finish(weight, own, gap, came, rows * planes * members)
    return new_weight, alpha, gap[0], top


def solution(mesh):
    fine = Mesh(mesh.devices.reshape(4, 4, 4, 2, 2), (ZH, X, Y, ZL, CORE))
    return jax.shard_map(
        round_of_ascent,
        mesh=fine,
        in_specs=(P(SAMP, None), P(SAMP), P(SAMP, CLS), P(SAMP, CLS), P(SAMP, None, None)),
        out_specs=(P(SAMP, CLS), P(SAMP, CLS), P(CLS), P(SAMP)),
        check_vma=False,
    )
```

```python
import functools

import jax
import jax.numpy as jnp
from jax import lax
from jax.experimental import pallas as pl
from jax.experimental.pallas import tpu as pltpu
from jax.sharding import Mesh, PartitionSpec as P


BLOCK = 16
PASSES = 2
COUPLING = 0.5

ZH, X, Y, ZL, CORE = "zh", "x", "y", "zl", "core"
PLANE = (X, Y)
SAMP = (ZH, X, Y)
CLS = (ZL, CORE)
GAP_ROWS = 8
EARLY = 10
ORDER = (0, 2, 1, 3)
F32, BF16 = jnp.float32, jnp.bfloat16
IN_VMEM = pl.BlockSpec(memory_space=pltpu.VMEM)
IN_SMEM = pl.BlockSpec(memory_space=pltpu.SMEM)
IN_HBM = pl.BlockSpec(memory_space=pltpu.HBM)
LEFT = (0, 0, 1, 1, 0, 2)
RIGHT = (0, 1, 0, 1, 2, 0)
SMALL = pltpu.CompilerParams(vmem_limit_bytes=16 * 2**20)
FULL = pltpu.CompilerParams(vmem_limit_bytes=60 * 1024 * 1024)


def shifted(value, axis, by):
    size = lax.axis_size(axis)
    return lax.ppermute(value, axis, [(i, (i + by) % size) for i in range(size)])


def pack_kernel(where, plane, rows_hbm, out_hbm, held_ref, in_sems, out_sems):
    members, part, total = out_hbm.shape
    planes = in_sems.shape[0]
    width = total // planes
    span = members * width
    row = pl.multiple_of(where[0] * part, part)
    loads = []
    for k in range(planes):
        low = pl.multiple_of(lax.rem(plane[0] + (planes - k), planes) * span, span)
        loads.append(pltpu.make_async_copy(rows_hbm.at[pl.ds(row, part), pl.ds(low, span)], held_ref.at[k], in_sems.at[k]))
    for load in loads:
        load.start()
    stores = []
    for k in range(planes):
        loads[k].wait()
        for place in range(members):
            store = pltpu.make_async_copy(
                held_ref.at[k, :, pl.ds(place * width, width)],
                out_hbm.at[place, :, pl.ds(k * width, width)],
                out_sems.at[k * members + place],
            )
            store.start()
            stores.append(store)
    for store in stores:
        store.wait()


def pack(samples, where, plane, planes, members, quarters):
    rows, features = samples.shape
    part = rows // quarters
    return pl.pallas_call(
        pack_kernel,
        in_specs=[IN_SMEM, IN_SMEM, IN_HBM],
        out_specs=IN_HBM,
        out_shape=jax.ShapeDtypeStruct((members, part, features // members), samples.dtype),
        scratch_shapes=[
            pltpu.VMEM((planes, part, features // planes), samples.dtype),
            pltpu.SemaphoreType.DMA((planes,)),
            pltpu.SemaphoreType.DMA((planes * members,)),
        ],
        compiler_params=FULL,
        name="pack",
    )(where, plane, samples)


def three_pieces(value):
    first = value.astype(BF16)
    rest = value - first.astype(F32)
    second = rest.astype(BF16)
    third = (rest - second.astype(F32)).astype(BF16)
    return first, second, third


def prepare_kernel(gram_ref, inverse_ref, expanded_ref, wide_ref):
    rows = gram_ref.shape[0]
    _, size, _ = inverse_ref.shape
    lanes = expanded_ref.shape[3]
    b = pl.program_id(0)
    low = pl.multiple_of(b * size, size)
    high = pl.multiple_of(lax.rem(b + 1, pl.num_programs(0)) * size, size)
    spot = lax.broadcasted_iota(jnp.int32, (rows, size), 0) == low + lax.broadcasted_iota(jnp.int32, (rows, size), 1)
    picks = jnp.where(spot, 1.0, 0.0).astype(BF16)
    sides = [jnp.dot(piece, picks, preferred_element_type=F32) for piece in three_pieces(COUPLING * gram_ref[...])]
    exact = jnp.dot(gram_ref[pl.ds(high, size)], jnp.where(spot, 1.0, 0.0), precision=lax.Precision.HIGHEST, preferred_element_type=F32)
    for k in range(size):
        expanded_ref[0, k] = jnp.broadcast_to(inverse_ref[0, :, k:k + 1], (size, lanes))
        expanded_ref[0, size + k] = COUPLING * jnp.broadcast_to(exact[:, k:k + 1], (size, lanes))
    wide_ref[0] = jnp.concatenate([sides[p].astype(BF16) for p in LEFT], axis=1)


def prepare(gram, inverse, lanes):
    rows = gram.shape[0]
    blocks, size, _ = inverse.shape
    return pl.pallas_call(
        prepare_kernel,
        grid=(blocks,),
        in_specs=[pl.BlockSpec((rows, rows), lambda b: (0, 0)), pl.BlockSpec((1, size, size), lambda b: (b, 0, 0))],
        out_specs=[
            pl.BlockSpec((1, 2 * size, size, lanes), lambda b: (b, 0, 0, 0)),
            pl.BlockSpec((1, rows, len(LEFT) * size), lambda b: (b, 0, 0)),
        ],
        out_shape=[
            jax.ShapeDtypeStruct((blocks, 2 * size, size, lanes), F32),
            jax.ShapeDtypeStruct((blocks, rows, len(LEFT) * size), BF16),
        ],
        compiler_params=FULL,
        name="prepare",
    )(gram, inverse)


def rows_product(expanded, value):
    size = value.shape[0]
    sums = []
    for k in range(size):
        term = expanded[k] * jnp.broadcast_to(value[k:k + 1], value.shape)
        if k < 4:
            sums.append(term)
        else:
            sums[k % 4] += term
    return (sums[0] + sums[1]) + (sums[2] + sums[3])


def passes_kernel(where, start0, start1, start2, start3, labels_hbm, dual_hbm, expanded_hbm, wide_hbm, alpha_hbm, steps_hbm, top_hbm,
                  margin_ref, labels_ref, dual_ref, expanded_ref, wide_ref, alpha_ref, start_ref, sign_ref, change_ref, payload_ref, top_ref, sems):
    rows, width = margin_ref.shape
    blocks = rows // BLOCK
    copies = [
        pltpu.make_async_copy(labels_hbm, labels_ref, sems.at[0]),
        pltpu.make_async_copy(dual_hbm, dual_ref, sems.at[1]),
    ]
    for d, piece in enumerate((start0, start1, start2, start3)):
        part = piece.shape[0]
        low = pl.multiple_of(lax.bitwise_xor(where[0], d) * part, part)
        copies.append(pltpu.make_async_copy(piece, start_ref.at[pl.ds(low, part)], sems.at[2 + d]))
    parts = [
        [pltpu.make_async_copy(expanded_hbm.at[b], expanded_ref.at[b], sems.at[6 + b]),
         pltpu.make_async_copy(wide_hbm.at[b], wide_ref.at[b], sems.at[6 + blocks + b])]
        for b in range(blocks)
    ]
    for copy in copies + [part for pair in parts for part in pair]:
        copy.start()
    change_ref[...] = jnp.zeros((rows, width), F32)
    for copy in copies:
        copy.wait()
    class_ids = where[0] * width + lax.broadcasted_iota(jnp.int32, (rows, width), 1)
    sign_ref[...] = jnp.where(labels_ref[...] == class_ids, 1.0, -1.0).astype(F32)
    margin_ref[...] = start_ref[...]
    alpha_ref[...] = dual_ref[...]
    margin = start_ref[:BLOCK]
    for turn in range(PASSES * blocks):
        b = turn % blocks
        at = slice(b * BLOCK, (b + 1) * BLOCK)
        n = (b + 1) % blocks
        if turn < blocks:
            for copy in parts[b]:
                copy.wait()
        signs = sign_ref[at]
        ascent = rows_product(expanded_ref[b, :BLOCK], 1.0 - signs * margin)
        alpha = jnp.clip(alpha_ref[at] + ascent, 0.0, 1.0)
        change = signs * (alpha - dual_ref[at])
        moved = change - change_ref[at]
        alpha_ref[at] = alpha
        change_ref[at] = change
        margin = margin_ref[n * BLOCK:(n + 1) * BLOCK] + rows_product(expanded_ref[b, BLOCK:], moved)
        pieces = three_pieces(moved)
        tall = jnp.concatenate([pieces[p] for p in RIGHT], axis=0)
        margin_ref[...] += jnp.dot(wide_ref[b], tall, preferred_element_type=F32)
    scaled = sign_ref[...] * start_ref[...]
    gap = jnp.sum(jnp.maximum(0.0, 1.0 - scaled) + dual_ref[...] * (scaled - 1.0), axis=0, keepdims=True)
    payload_ref[:rows] = change_ref[...].astype(BF16)
    payload_ref[rows:] = tail_of(gap)
    outs = [pltpu.make_async_copy(payload_ref, steps_hbm.at[place], sems.at[place]) for place in range(steps_hbm.shape[0])]
    for copy in outs:
        copy.start()
    top_ref[...] = jnp.max(margin_ref[...].T, axis=0, keepdims=True)
    after = steps_hbm.shape[0]
    outs += [pltpu.make_async_copy(alpha_ref, alpha_hbm, sems.at[after]), pltpu.make_async_copy(top_ref, top_hbm, sems.at[after + 1])]
    for copy in outs[after:]:
        copy.start()
    for copy in outs:
        copy.wait()


def passes(where, start, labels, dual, ready, members):
    rows, width = dual.shape
    square = pltpu.VMEM((rows, width), F32)
    return pl.pallas_call(
        passes_kernel,
        in_specs=[IN_SMEM] + [IN_HBM] * (len(start) + 4),
        out_specs=[IN_HBM] * 3,
        out_shape=[
            jax.ShapeDtypeStruct((rows, width), F32),
            jax.ShapeDtypeStruct((members, rows + GAP_ROWS, width), BF16),
            jax.ShapeDtypeStruct((1, rows), F32),
        ],
        scratch_shapes=[
            square,
            pltpu.VMEM(labels.shape, labels.dtype),
            square,
            pltpu.VMEM(ready[0].shape, ready[0].dtype),
            pltpu.VMEM(ready[1].shape, ready[1].dtype),
            square,
            square,
            square,
            square,
            pltpu.VMEM((rows + GAP_ROWS, width), BF16),
            pltpu.VMEM((1, rows), F32),
            pltpu.SemaphoreType.DMA((6 + 2 * (rows // BLOCK),)),
        ],
        compiler_params=FULL,
        name="passes",
    )(where, *start, labels, dual, *ready)


def tail_of(gap):
    first, second, third = three_pieces(gap)
    row = lax.broadcasted_iota(jnp.int32, (GAP_ROWS, gap.shape[1]), 0)
    zero = jnp.zeros((GAP_ROWS, gap.shape[1]), F32)
    return jnp.where(row == 0, first.astype(F32), jnp.where(row == 1, second.astype(F32), jnp.where(row == 2, third.astype(F32), zero))).astype(BF16)


def from_tail(tail):
    tail = tail.astype(F32)
    return (tail[0:1] + tail[1:2]) + tail[2:3]


def fetches(held_refs, block_ref, sems, k):
    depth = block_ref.shape[1]
    copies, low = [], 0
    for i, ref in enumerate(held_refs):
        rows = ref.shape[0]
        copies.append(pltpu.make_async_copy(ref.at[:, pl.ds(k * depth, depth)], block_ref.at[pl.ds(low, rows)], sems.at[i]))
        low += rows
    for copy in copies:
        copy.start()
    return copies


def lanes_of(rows):
    return -(-rows // 128) * 128


def product(turned_ref, block_ref, copies, heights):
    total, low, at = None, 0, 0
    for copy, rows in zip(copies, heights):
        copy.wait()
        term = jnp.dot(turned_ref[:, at:at + rows], block_ref[low:low + rows], preferred_element_type=F32)
        total = term if total is None else total + term
        low += rows
        at += lanes_of(rows)
    return total.T


def first_delta_kernel(k, where, *refs):
    *held, steps_ref, sent_ref, turned_ref, gap_ref, block_ref, sems = refs
    copies = fetches(held, block_ref, sems, k)
    members, tall, width = steps_ref.shape
    rows = tall - GAP_ROWS
    part = rows // len(ORDER)
    d, first, at = 0, 0, 0
    for ref in held:
        count = ref.shape[0] // part
        low = pl.multiple_of(lax.bitwise_xor(where[0], d) * part, part)
        picked = jnp.concatenate([steps_ref[g, pl.ds(low, part), :] for g in range(first, first + count)], axis=0)
        turned_ref[:, at:at + count * part] = picked.astype(F32).T.astype(BF16)
        at += lanes_of(count * part)
        d, first = (d + 1, 0) if first + count == members else (d, first + count)
    gap = jnp.zeros((1, width), F32)
    for g in range(members):
        gap += from_tail(steps_ref[g, rows:, :])
    gap_ref[...] = gap
    delta = product(turned_ref, block_ref, copies, [ref.shape[0] for ref in held])
    depth = delta.shape[0]
    sent_ref[:depth] = delta.astype(BF16)
    sent_ref[depth:] = tail_of(gap)


def next_delta_kernel(k, *refs):
    *held, turned_ref, gap_ref, sent_ref, block_ref, sems = refs
    copies = fetches(held, block_ref, sems, k)
    delta = product(turned_ref, block_ref, copies, [ref.shape[0] for ref in held])
    depth = delta.shape[0]
    sent_ref[:depth] = delta.astype(BF16)
    sent_ref[depth:] = tail_of(gap_ref[...])


def own_delta_kernel(*refs):
    *held, turned_ref, sum_ref, block_ref, sems = refs
    copies = fetches(held, block_ref, sems, 0)
    sum_ref[...] = product(turned_ref, block_ref, copies, [ref.shape[0] for ref in held])


def finish_kernel(count, weight_ref, own_ref, gap_ref, *refs):
    *came, new_ref, class_gap_ref = refs
    depth = own_ref.shape[0]
    total, gap = own_ref[...], gap_ref[...]
    for ref in came:
        total += ref[:depth].astype(F32)
        gap += from_tail(ref[depth:])
    new_ref[...] = weight_ref[...].astype(F32) + COUPLING * total
    class_gap_ref[...] = gap / count


def finish(weight, own, gap, came, count):
    depth, width = weight.shape
    whole = pl.BlockSpec(memory_space=pltpu.VMEM)
    return pl.pallas_call(
        functools.partial(finish_kernel, count),
        in_specs=[whole] * (3 + len(came)),
        out_specs=[whole] * 2,
        out_shape=[jax.ShapeDtypeStruct((depth, width), F32), jax.ShapeDtypeStruct((1, width), F32)],
        compiler_params=SMALL,
        name="finish",
    )(weight, own, gap, *came)


def block_scratch(quarters, planes):
    rows = sum(held.shape[0] for held in quarters)
    return [pltpu.VMEM((rows, quarters[0].shape[1] // planes), BF16), pltpu.SemaphoreType.DMA((len(quarters),))]


def first_delta(where, quarters, steps, planes, k):
    features = quarters[0].shape[1]
    width = steps.shape[2]
    return pl.pallas_call(
        functools.partial(first_delta_kernel, k),
        in_specs=[IN_SMEM] + [IN_HBM] * len(quarters) + [IN_VMEM],
        out_specs=[IN_VMEM] * 3,
        out_shape=[
            jax.ShapeDtypeStruct((features // planes + GAP_ROWS, width), BF16),
            jax.ShapeDtypeStruct((width, sum(lanes_of(held.shape[0]) for held in quarters)), BF16),
            jax.ShapeDtypeStruct((1, width), F32),
        ],
        scratch_shapes=block_scratch(quarters, planes),
        compiler_params=SMALL,
        name="delta_first",
    )(where, *quarters, steps)


def next_delta(quarters, turned, gap, planes, k):
    return pl.pallas_call(
        functools.partial(next_delta_kernel, k),
        in_specs=[IN_HBM] * len(quarters) + [IN_VMEM] * 2,
        out_specs=IN_VMEM,
        out_shape=jax.ShapeDtypeStruct((quarters[0].shape[1] // planes + GAP_ROWS, gap.shape[1]), BF16),
        scratch_shapes=block_scratch(quarters, planes),
        compiler_params=SMALL,
        name="delta_next",
    )(*quarters, turned, gap)


def own_delta(quarters, turned, planes):
    return pl.pallas_call(
        own_delta_kernel,
        in_specs=[IN_HBM] * len(quarters) + [IN_VMEM],
        out_specs=IN_VMEM,
        out_shape=jax.ShapeDtypeStruct((quarters[0].shape[1] // planes, turned.shape[0]), F32),
        scratch_shapes=block_scratch(quarters, planes),
        compiler_params=SMALL,
        name="delta_own",
    )(*quarters, turned)


def gathered_kernel(parts_hbm, *refs):
    *outs, parts_ref, sems = refs
    width = outs[0].shape[1]
    copies = [pltpu.make_async_copy(parts_hbm.at[g], parts_ref.at[g], sems.at[g]) for g in range(parts_hbm.shape[0])]
    for copy in copies:
        copy.start()
    copies[0].wait()
    total = parts_ref[0]
    for g in range(1, len(copies)):
        copies[g].wait()
        total += parts_ref[g]
    for i, d in enumerate(ORDER):
        outs[d][...] = total[:, i * width:(i + 1) * width]


def gathered(parts):
    members, part, total = parts.shape
    return pl.pallas_call(
        gathered_kernel,
        in_specs=[IN_HBM],
        out_specs=[IN_VMEM] * len(ORDER),
        out_shape=[jax.ShapeDtypeStruct((part, total // len(ORDER)), F32)] * len(ORDER),
        scratch_shapes=[pltpu.VMEM(parts.shape, F32), pltpu.SemaphoreType.DMA((members,))],
        compiler_params=FULL,
        name="gathered",
    )(parts)


def self_product(value):
    return lax.dot_general(value, value, (((1,), (1,)), ((), ())), preferred_element_type=F32)


def round_of_ascent(samples, labels, weight, dual, inverse):
    rows = samples.shape[0]
    depth, width = weight.shape
    planes = lax.axis_size(ZH)
    members = lax.axis_size(X) * lax.axis_size(Y)
    quarters = lax.axis_size(ZL) * lax.axis_size(CORE)
    part = rows // quarters
    mine = lax.axis_index(CLS).astype(jnp.int32)
    where = mine.reshape(1)
    plane = lax.axis_index(ZH).astype(jnp.int32).reshape(1)

    packed = pack(samples, where, plane, planes, members, quarters)
    quarter = lax.all_to_all(packed, PLANE, split_axis=0, concat_axis=0, tiled=True)
    from_below = shifted(weight, ZH, 1)
    from_above = shifted(weight, ZH, -1)
    far_head = shifted(from_below[:depth // 2], ZH, 1)
    far_rest = shifted(from_above[depth // 2:], ZH, -1)
    near = [weight, from_below, jnp.concatenate([far_head, far_rest], axis=0), from_above]
    lines = []
    for k in range(planes):
        lines.append(shifted(near[k], ZL, 1))
    by_pair = jnp.concatenate([jnp.concatenate(pair, axis=1) for pair in zip(near, lines)], axis=0)
    by_all = jnp.concatenate([by_pair, shifted(by_pair, CORE, 1)], axis=1)
    middle = samples.shape[1] // 2
    gram_head = self_product(samples[:, :middle])

    flat = quarter.reshape(members * part, planes * depth)
    early = members * EARLY // 16 * part
    beside_a = shifted(flat[:early], ZL, 1)
    partial = jnp.dot(flat, by_all, preferred_element_type=F32)
    partial, late = lax.optimization_barrier((partial, flat))
    partial = lax.all_to_all(partial.reshape(members, part, quarters * width), PLANE, split_axis=0, concat_axis=0, tiled=True)
    across = shifted(flat, CORE, 1)
    diagonal_a = shifted(beside_a, CORE, 1)
    gram = gram_head + self_product(samples[:, middle:])
    ready = prepare(gram, inverse, width)
    partial, late, tags = lax.optimization_barrier((partial, late[early:], labels[:, None]))
    own_piece, by_core, by_line, by_both = gathered(partial)
    by_line = shifted(by_line, ZL, 1)
    by_both = lax.ppermute(by_both, CLS, [(i, i ^ 3) for i in range(4)])
    by_core = shifted(by_core, CORE, 1)
    start = [own_piece, by_core, by_line, by_both]
    beside_b = shifted(late, ZL, 1)

    alpha, steps, top = passes(where, start, tags, dual, ready, members)
    steps = lax.all_to_all(steps, PLANE, split_axis=0, concat_axis=0, tiled=True)
    diagonal_b = shifted(beside_b, CORE, 1)

    top = top[0]
    other = shifted(top, CORE, 1)
    top = jnp.maximum(top, other)
    other = shifted(top, ZL, 1)
    top = jnp.maximum(top, other)

    held = [flat, across, beside_a, beside_b, diagonal_a, diagonal_b]
    far = planes // 2
    sent, turned, gap = first_delta(where, held, steps, planes, far)
    came = [shifted(sent, ZH, planes - far)]
    for k in range(1, planes):
        if k != far:
            sent = next_delta(held, turned, gap, planes, k)
            came.append(shifted(sent, ZH, planes - k))
    own = own_delta(held, turned, planes)
    new_weight, gap = finish(weight, own, gap, came, rows * planes * members)
    return new_weight, alpha, gap[0], top


def solution(mesh):
    fine = Mesh(mesh.devices.reshape(4, 4, 4, 2, 2), (ZH, X, Y, ZL, CORE))
    return jax.shard_map(
        round_of_ascent,
        mesh=fine,
        in_specs=(P(SAMP, None), P(SAMP), P(SAMP, CLS), P(SAMP, CLS), P(SAMP, None, None)),
        out_specs=(P(SAMP, CLS), P(SAMP, CLS), P(CLS), P(SAMP)),
        check_vma=False,
    )
```

```python
import functools

import jax
import jax.numpy as jnp
from jax import lax
from jax.experimental import pallas as pl
from jax.experimental.pallas import tpu as pltpu
from jax.sharding import Mesh, PartitionSpec as P


BLOCK = 16
PASSES = 2
COUPLING = 0.5

ZH, X, Y, ZL, CORE = "zh", "x", "y", "zl", "core"
PLANE = (X, Y)
SAMP = (ZH, X, Y)
CLS = (ZL, CORE)
GAP_ROWS = 8
EARLY = 10
ORDER = (0, 2, 1, 3)
F32, BF16 = jnp.float32, jnp.bfloat16
IN_VMEM = pl.BlockSpec(memory_space=pltpu.VMEM)
IN_SMEM = pl.BlockSpec(memory_space=pltpu.SMEM)
IN_HBM = pl.BlockSpec(memory_space=pltpu.HBM)
LEFT = (0, 0, 1, 1, 0, 2)
RIGHT = (0, 1, 0, 1, 2, 0)
SMALL = pltpu.CompilerParams(vmem_limit_bytes=16 * 2**20)
FULL = pltpu.CompilerParams(vmem_limit_bytes=60 * 1024 * 1024)


def shifted(value, axis, by):
    size = lax.axis_size(axis)
    return lax.ppermute(value, axis, [(i, (i + by) % size) for i in range(size)])


def pack_kernel(where, plane, rows_hbm, out_hbm, held_ref, in_sems, out_sems):
    members, part, total = out_hbm.shape
    planes = in_sems.shape[0]
    width = total // planes
    span = members * width
    row = pl.multiple_of(where[0] * part, part)
    loads = []
    for k in range(planes):
        low = pl.multiple_of(lax.rem(plane[0] + (planes - k), planes) * span, span)
        loads.append(pltpu.make_async_copy(rows_hbm.at[pl.ds(row, part), pl.ds(low, span)], held_ref.at[k], in_sems.at[k]))
    for load in loads:
        load.start()
    stores = []
    for k in range(planes):
        loads[k].wait()
        for place in range(members):
            store = pltpu.make_async_copy(
                held_ref.at[k, :, pl.ds(place * width, width)],
                out_hbm.at[place, :, pl.ds(k * width, width)],
                out_sems.at[k * members + place],
            )
            store.start()
            stores.append(store)
    for store in stores:
        store.wait()


def pack(samples, where, plane, planes, members, quarters):
    rows, features = samples.shape
    part = rows // quarters
    return pl.pallas_call(
        pack_kernel,
        in_specs=[IN_SMEM, IN_SMEM, IN_HBM],
        out_specs=IN_HBM,
        out_shape=jax.ShapeDtypeStruct((members, part, features // members), samples.dtype),
        scratch_shapes=[
            pltpu.VMEM((planes, part, features // planes), samples.dtype),
            pltpu.SemaphoreType.DMA((planes,)),
            pltpu.SemaphoreType.DMA((planes * members,)),
        ],
        compiler_params=FULL,
        name="pack",
    )(where, plane, samples)


def three_pieces(value):
    first = value.astype(BF16)
    rest = value - first.astype(F32)
    second = rest.astype(BF16)
    third = (rest - second.astype(F32)).astype(BF16)
    return first, second, third


def prepare_kernel(gram_ref, inverse_ref, expanded_ref, wide_ref):
    rows = gram_ref.shape[0]
    _, size, _ = inverse_ref.shape
    lanes = expanded_ref.shape[3]
    b = pl.program_id(0)
    low = pl.multiple_of(b * size, size)
    high = pl.multiple_of(lax.rem(b + 1, pl.num_programs(0)) * size, size)
    spot = lax.broadcasted_iota(jnp.int32, (rows, size), 0) == low + lax.broadcasted_iota(jnp.int32, (rows, size), 1)
    picks = jnp.where(spot, 1.0, 0.0).astype(BF16)
    sides = [jnp.dot(piece, picks, preferred_element_type=F32) for piece in three_pieces(COUPLING * gram_ref[...])]
    exact = jnp.dot(gram_ref[pl.ds(high, size)], jnp.where(spot, 1.0, 0.0), precision=lax.Precision.HIGHEST, preferred_element_type=F32)
    for k in range(size):
        expanded_ref[0, k] = jnp.broadcast_to(inverse_ref[0, :, k:k + 1], (size, lanes))
        expanded_ref[0, size + k] = COUPLING * jnp.broadcast_to(exact[:, k:k + 1], (size, lanes))
    wide_ref[0] = jnp.concatenate([sides[p].astype(BF16) for p in LEFT], axis=1)


def prepare(gram, inverse, lanes):
    rows = gram.shape[0]
    blocks, size, _ = inverse.shape
    return pl.pallas_call(
        prepare_kernel,
        grid=(blocks,),
        in_specs=[pl.BlockSpec((rows, rows), lambda b: (0, 0)), pl.BlockSpec((1, size, size), lambda b: (b, 0, 0))],
        out_specs=[
            pl.BlockSpec((1, 2 * size, size, lanes), lambda b: (b, 0, 0, 0)),
            pl.BlockSpec((1, rows, len(LEFT) * size), lambda b: (b, 0, 0)),
        ],
        out_shape=[
            jax.ShapeDtypeStruct((blocks, 2 * size, size, lanes), F32),
            jax.ShapeDtypeStruct((blocks, rows, len(LEFT) * size), BF16),
        ],
        compiler_params=FULL,
        name="prepare",
    )(gram, inverse)


def rows_product(expanded, value):
    size = value.shape[0]
    sums = []
    for k in range(size):
        term = expanded[k] * jnp.broadcast_to(value[k:k + 1], value.shape)
        if k < 4:
            sums.append(term)
        else:
            sums[k % 4] += term
    return (sums[0] + sums[1]) + (sums[2] + sums[3])


def passes_kernel(where, start0, start1, start2, start3, labels_hbm, dual_hbm, expanded_hbm, wide_hbm, alpha_hbm, steps_hbm, top_hbm,
                  margin_ref, labels_ref, dual_ref, expanded_ref, wide_ref, alpha_ref, start_ref, sign_ref, change_ref, payload_ref, top_ref, sems):
    rows, width = margin_ref.shape
    blocks = rows // BLOCK
    copies = [
        pltpu.make_async_copy(labels_hbm, labels_ref, sems.at[0]),
        pltpu.make_async_copy(dual_hbm, dual_ref, sems.at[1]),
    ]
    for d, piece in enumerate((start0, start1, start2, start3)):
        part = piece.shape[0]
        low = pl.multiple_of(lax.bitwise_xor(where[0], d) * part, part)
        copies.append(pltpu.make_async_copy(piece, start_ref.at[pl.ds(low, part)], sems.at[2 + d]))
    parts = [
        [pltpu.make_async_copy(expanded_hbm.at[b], expanded_ref.at[b], sems.at[6 + b]),
         pltpu.make_async_copy(wide_hbm.at[b], wide_ref.at[b], sems.at[6 + blocks + b])]
        for b in range(blocks)
    ]
    for copy in copies + [part for pair in parts for part in pair]:
        copy.start()
    change_ref[...] = jnp.zeros((rows, width), F32)
    for copy in copies:
        copy.wait()
    class_ids = where[0] * width + lax.broadcasted_iota(jnp.int32, (rows, width), 1)
    tags = jnp.broadcast_to(labels_ref[...].astype(F32), (width, rows)).T
    sign_ref[...] = jnp.where(tags == class_ids.astype(F32), 1.0, -1.0)
    margin_ref[...] = start_ref[...]
    alpha_ref[...] = dual_ref[...]
    margin = start_ref[:BLOCK]
    for turn in range(PASSES * blocks):
        b = turn % blocks
        at = slice(b * BLOCK, (b + 1) * BLOCK)
        n = (b + 1) % blocks
        if turn < blocks:
            for copy in parts[b]:
                copy.wait()
        signs = sign_ref[at]
        ascent = rows_product(expanded_ref[b, :BLOCK], 1.0 - signs * margin)
        alpha = jnp.clip(alpha_ref[at] + ascent, 0.0, 1.0)
        change = signs * (alpha - dual_ref[at])
        moved = change - change_ref[at]
        alpha_ref[at] = alpha
        change_ref[at] = change
        margin = margin_ref[n * BLOCK:(n + 1) * BLOCK] + rows_product(expanded_ref[b, BLOCK:], moved)
        pieces = three_pieces(moved)
        tall = jnp.concatenate([pieces[p] for p in RIGHT], axis=0)
        margin_ref[...] += jnp.dot(wide_ref[b], tall, preferred_element_type=F32)
    scaled = sign_ref[...] * start_ref[...]
    gap = jnp.sum(jnp.maximum(0.0, 1.0 - scaled) + dual_ref[...] * (scaled - 1.0), axis=0, keepdims=True)
    payload_ref[:rows] = change_ref[...].astype(BF16)
    payload_ref[rows:] = tail_of(gap)
    outs = [pltpu.make_async_copy(payload_ref, steps_hbm.at[place], sems.at[place]) for place in range(steps_hbm.shape[0])]
    for copy in outs:
        copy.start()
    top_ref[...] = jnp.max(margin_ref[...].T, axis=0, keepdims=True)
    after = steps_hbm.shape[0]
    outs += [pltpu.make_async_copy(alpha_ref, alpha_hbm, sems.at[after]), pltpu.make_async_copy(top_ref, top_hbm, sems.at[after + 1])]
    for copy in outs[after:]:
        copy.start()
    for copy in outs:
        copy.wait()


def passes(where, start, labels, dual, ready, members):
    rows, width = dual.shape
    square = pltpu.VMEM((rows, width), F32)
    return pl.pallas_call(
        passes_kernel,
        in_specs=[IN_SMEM] + [IN_HBM] * (len(start) + 4),
        out_specs=[IN_HBM] * 3,
        out_shape=[
            jax.ShapeDtypeStruct((rows, width), F32),
            jax.ShapeDtypeStruct((members, rows + GAP_ROWS, width), BF16),
            jax.ShapeDtypeStruct((1, rows), F32),
        ],
        scratch_shapes=[
            square,
            pltpu.VMEM(labels.shape, labels.dtype),
            square,
            pltpu.VMEM(ready[0].shape, ready[0].dtype),
            pltpu.VMEM(ready[1].shape, ready[1].dtype),
            square,
            square,
            square,
            square,
            pltpu.VMEM((rows + GAP_ROWS, width), BF16),
            pltpu.VMEM((1, rows), F32),
            pltpu.SemaphoreType.DMA((6 + 2 * (rows // BLOCK),)),
        ],
        compiler_params=FULL,
        name="passes",
    )(where, *start, labels, dual, *ready)


def tail_of(gap):
    first, second, third = three_pieces(gap)
    row = lax.broadcasted_iota(jnp.int32, (GAP_ROWS, gap.shape[1]), 0)
    zero = jnp.zeros((GAP_ROWS, gap.shape[1]), F32)
    return jnp.where(row == 0, first.astype(F32), jnp.where(row == 1, second.astype(F32), jnp.where(row == 2, third.astype(F32), zero))).astype(BF16)


def from_tail(tail):
    tail = tail.astype(F32)
    return (tail[0:1] + tail[1:2]) + tail[2:3]


def fetches(held_refs, block_ref, sems, k):
    depth = block_ref.shape[1]
    copies, low = [], 0
    for i, ref in enumerate(held_refs):
        rows = ref.shape[0]
        copies.append(pltpu.make_async_copy(ref.at[:, pl.ds(k * depth, depth)], block_ref.at[pl.ds(low, rows)], sems.at[i]))
        low += rows
    for copy in copies:
        copy.start()
    return copies


def lanes_of(rows):
    return -(-rows // 128) * 128


def product(turned_ref, block_ref, copies, heights):
    total, low, at = None, 0, 0
    for copy, rows in zip(copies, heights):
        copy.wait()
        term = jnp.dot(turned_ref[:, at:at + rows], block_ref[low:low + rows], preferred_element_type=F32)
        total = term if total is None else total + term
        low += rows
        at += lanes_of(rows)
    return total.T


def first_delta_kernel(k, where, *refs):
    *held, steps_ref, sent_ref, turned_ref, gap_ref, block_ref, sems = refs
    copies = fetches(held, block_ref, sems, k)
    members, tall, width = steps_ref.shape
    rows = tall - GAP_ROWS
    part = rows // len(ORDER)
    d, first, at = 0, 0, 0
    for ref in held:
        count = ref.shape[0] // part
        low = pl.multiple_of(lax.bitwise_xor(where[0], d) * part, part)
        picked = jnp.concatenate([steps_ref[g, pl.ds(low, part), :] for g in range(first, first + count)], axis=0)
        turned_ref[:, at:at + count * part] = picked.astype(F32).T.astype(BF16)
        at += lanes_of(count * part)
        d, first = (d + 1, 0) if first + count == members else (d, first + count)
    gap = jnp.zeros((1, width), F32)
    for g in range(members):
        gap += from_tail(steps_ref[g, rows:, :])
    gap_ref[...] = gap
    delta = product(turned_ref, block_ref, copies, [ref.shape[0] for ref in held])
    depth = delta.shape[0]
    sent_ref[:depth] = delta.astype(BF16)
    sent_ref[depth:] = tail_of(gap)


def next_delta_kernel(k, *refs):
    *held, turned_ref, gap_ref, sent_ref, block_ref, sems = refs
    copies = fetches(held, block_ref, sems, k)
    delta = product(turned_ref, block_ref, copies, [ref.shape[0] for ref in held])
    depth = delta.shape[0]
    sent_ref[:depth] = delta.astype(BF16)
    sent_ref[depth:] = tail_of(gap_ref[...])


def own_delta_kernel(*refs):
    *held, turned_ref, sum_ref, block_ref, sems = refs
    copies = fetches(held, block_ref, sems, 0)
    sum_ref[...] = product(turned_ref, block_ref, copies, [ref.shape[0] for ref in held])


def finish_kernel(count, weight_ref, own_ref, gap_ref, *refs):
    *came, new_ref, class_gap_ref = refs
    depth = own_ref.shape[0]
    total, gap = own_ref[...], gap_ref[...]
    for ref in came:
        total += ref[:depth].astype(F32)
        gap += from_tail(ref[depth:])
    new_ref[...] = weight_ref[...].astype(F32) + COUPLING * total
    class_gap_ref[...] = gap / count


def finish(weight, own, gap, came, count):
    depth, width = weight.shape
    whole = pl.BlockSpec(memory_space=pltpu.VMEM)
    return pl.pallas_call(
        functools.partial(finish_kernel, count),
        in_specs=[whole] * (3 + len(came)),
        out_specs=[whole] * 2,
        out_shape=[jax.ShapeDtypeStruct((depth, width), F32), jax.ShapeDtypeStruct((1, width), F32)],
        compiler_params=SMALL,
        name="finish",
    )(weight, own, gap, *came)


def block_scratch(quarters, planes):
    rows = sum(held.shape[0] for held in quarters)
    return [pltpu.VMEM((rows, quarters[0].shape[1] // planes), BF16), pltpu.SemaphoreType.DMA((len(quarters),))]


def first_delta(where, quarters, steps, planes, k):
    features = quarters[0].shape[1]
    width = steps.shape[2]
    return pl.pallas_call(
        functools.partial(first_delta_kernel, k),
        in_specs=[IN_SMEM] + [IN_HBM] * len(quarters) + [IN_VMEM],
        out_specs=[IN_VMEM] * 3,
        out_shape=[
            jax.ShapeDtypeStruct((features // planes + GAP_ROWS, width), BF16),
            jax.ShapeDtypeStruct((width, sum(lanes_of(held.shape[0]) for held in quarters)), BF16),
            jax.ShapeDtypeStruct((1, width), F32),
        ],
        scratch_shapes=block_scratch(quarters, planes),
        compiler_params=SMALL,
        name="delta_first",
    )(where, *quarters, steps)


def next_delta(quarters, turned, gap, planes, k):
    return pl.pallas_call(
        functools.partial(next_delta_kernel, k),
        in_specs=[IN_HBM] * len(quarters) + [IN_VMEM] * 2,
        out_specs=IN_VMEM,
        out_shape=jax.ShapeDtypeStruct((quarters[0].shape[1] // planes + GAP_ROWS, gap.shape[1]), BF16),
        scratch_shapes=block_scratch(quarters, planes),
        compiler_params=SMALL,
        name="delta_next",
    )(*quarters, turned, gap)


def own_delta(quarters, turned, planes):
    return pl.pallas_call(
        own_delta_kernel,
        in_specs=[IN_HBM] * len(quarters) + [IN_VMEM],
        out_specs=IN_VMEM,
        out_shape=jax.ShapeDtypeStruct((quarters[0].shape[1] // planes, turned.shape[0]), F32),
        scratch_shapes=block_scratch(quarters, planes),
        compiler_params=SMALL,
        name="delta_own",
    )(*quarters, turned)


def gathered_kernel(parts_hbm, *refs):
    *outs, parts_ref, sems = refs
    width = outs[0].shape[1]
    copies = [pltpu.make_async_copy(parts_hbm.at[g], parts_ref.at[g], sems.at[g]) for g in range(parts_hbm.shape[0])]
    for copy in copies:
        copy.start()
    copies[0].wait()
    total = parts_ref[0]
    for g in range(1, len(copies)):
        copies[g].wait()
        total += parts_ref[g]
    for i, d in enumerate(ORDER):
        outs[d][...] = total[:, i * width:(i + 1) * width]


def gathered(parts):
    members, part, total = parts.shape
    return pl.pallas_call(
        gathered_kernel,
        in_specs=[IN_HBM],
        out_specs=[IN_VMEM] * len(ORDER),
        out_shape=[jax.ShapeDtypeStruct((part, total // len(ORDER)), F32)] * len(ORDER),
        scratch_shapes=[pltpu.VMEM(parts.shape, F32), pltpu.SemaphoreType.DMA((members,))],
        compiler_params=FULL,
        name="gathered",
    )(parts)


def self_product(value):
    return lax.dot_general(value, value, (((1,), (1,)), ((), ())), preferred_element_type=F32)


def round_of_ascent(samples, labels, weight, dual, inverse):
    rows = samples.shape[0]
    depth, width = weight.shape
    planes = lax.axis_size(ZH)
    members = lax.axis_size(X) * lax.axis_size(Y)
    quarters = lax.axis_size(ZL) * lax.axis_size(CORE)
    part = rows // quarters
    mine = lax.axis_index(CLS).astype(jnp.int32)
    where = mine.reshape(1)
    plane = lax.axis_index(ZH).astype(jnp.int32).reshape(1)

    packed = pack(samples, where, plane, planes, members, quarters)
    quarter = lax.all_to_all(packed, PLANE, split_axis=0, concat_axis=0, tiled=True)
    from_below = shifted(weight, ZH, 1)
    from_above = shifted(weight, ZH, -1)
    far_head = shifted(from_below[:depth // 2], ZH, 1)
    far_rest = shifted(from_above[depth // 2:], ZH, -1)
    near = [weight, from_below, jnp.concatenate([far_head, far_rest], axis=0), from_above]
    lines = []
    for k in range(planes):
        lines.append(shifted(near[k], ZL, 1))
    by_pair = jnp.concatenate([jnp.concatenate(pair, axis=1) for pair in zip(near, lines)], axis=0)
    by_all = jnp.concatenate([by_pair, shifted(by_pair, CORE, 1)], axis=1)
    middle = samples.shape[1] // 2
    gram_head = self_product(samples[:, :middle])

    flat = quarter.reshape(members * part, planes * depth)
    early = members * EARLY // 16 * part
    beside_a = shifted(flat[:early], ZL, 1)
    partial = jnp.dot(flat, by_all, preferred_element_type=F32)
    partial, late = lax.optimization_barrier((partial, flat))
    partial = lax.all_to_all(partial.reshape(members, part, quarters * width), PLANE, split_axis=0, concat_axis=0, tiled=True)
    across = shifted(flat, CORE, 1)
    diagonal_a = shifted(beside_a, CORE, 1)
    gram = gram_head + self_product(samples[:, middle:])
    ready = prepare(gram, inverse, width)
    partial, late = lax.optimization_barrier((partial, late[early:]))
    own_piece, by_core, by_line, by_both = gathered(partial)
    by_line = shifted(by_line, ZL, 1)
    by_both = lax.ppermute(by_both, CLS, [(i, i ^ 3) for i in range(4)])
    by_core = shifted(by_core, CORE, 1)
    start = [own_piece, by_core, by_line, by_both]
    beside_b = shifted(late, ZL, 1)

    alpha, steps, top = passes(where, start, labels[None, :], dual, ready, members)
    steps = lax.all_to_all(steps, PLANE, split_axis=0, concat_axis=0, tiled=True)
    diagonal_b = shifted(beside_b, CORE, 1)

    top = top[0]
    other = shifted(top, CORE, 1)
    top = jnp.maximum(top, other)
    other = shifted(top, ZL, 1)
    top = jnp.maximum(top, other)

    held = [flat, across, beside_a, beside_b, diagonal_a, diagonal_b]
    far = planes // 2
    sent, turned, gap = first_delta(where, held, steps, planes, far)
    came = [shifted(sent, ZH, planes - far)]
    for k in range(1, planes):
        if k != far:
            sent = next_delta(held, turned, gap, planes, k)
            came.append(shifted(sent, ZH, planes - k))
    own = own_delta(held, turned, planes)
    new_weight, gap = finish(weight, own, gap, came, rows * planes * members)
    return new_weight, alpha, gap[0], top


def solution(mesh):
    fine = Mesh(mesh.devices.reshape(4, 4, 4, 2, 2), (ZH, X, Y, ZL, CORE))
    return jax.shard_map(
        round_of_ascent,
        mesh=fine,
        in_specs=(P(SAMP, None), P(SAMP), P(SAMP, CLS), P(SAMP, CLS), P(SAMP, None, None)),
        out_specs=(P(SAMP, CLS), P(SAMP, CLS), P(CLS), P(SAMP)),
        check_vma=False,
    )
```

```python
import functools

import jax
import jax.numpy as jnp
from jax import lax
from jax.experimental import pallas as pl
from jax.experimental.pallas import tpu as pltpu
from jax.sharding import Mesh, PartitionSpec as P


BLOCK = 16
PASSES = 2
COUPLING = 0.5

ZH, X, Y, ZL, CORE = "zh", "x", "y", "zl", "core"
PLANE = (X, Y)
SAMP = (ZH, X, Y)
CLS = (ZL, CORE)
GAP_ROWS = 8
EARLY = 10
ORDER = (0, 2, 1, 3)
F32, BF16 = jnp.float32, jnp.bfloat16
IN_VMEM = pl.BlockSpec(memory_space=pltpu.VMEM)
IN_SMEM = pl.BlockSpec(memory_space=pltpu.SMEM)
IN_HBM = pl.BlockSpec(memory_space=pltpu.HBM)
LEFT = (0, 0, 1, 1, 0, 2)
RIGHT = (0, 1, 0, 1, 2, 0)
SMALL = pltpu.CompilerParams(vmem_limit_bytes=16 * 2**20)
FULL = pltpu.CompilerParams(vmem_limit_bytes=60 * 1024 * 1024)


def shifted(value, axis, by):
    size = lax.axis_size(axis)
    return lax.ppermute(value, axis, [(i, (i + by) % size) for i in range(size)])


def pack_kernel(where, plane, rows_hbm, out_hbm, held_ref, in_sems, out_sems):
    members, part, total = out_hbm.shape
    planes = in_sems.shape[0]
    width = total // planes
    span = members * width
    row = pl.multiple_of(where[0] * part, part)
    loads = []
    for k in range(planes):
        low = pl.multiple_of(lax.rem(plane[0] + (planes - k), planes) * span, span)
        loads.append(pltpu.make_async_copy(rows_hbm.at[pl.ds(row, part), pl.ds(low, span)], held_ref.at[k], in_sems.at[k]))
    for load in loads:
        load.start()
    stores = []
    for k in range(planes):
        loads[k].wait()
        for place in range(members):
            store = pltpu.make_async_copy(
                held_ref.at[k, :, pl.ds(place * width, width)],
                out_hbm.at[place, :, pl.ds(k * width, width)],
                out_sems.at[k * members + place],
            )
            store.start()
            stores.append(store)
    for store in stores:
        store.wait()


def pack(samples, where, plane, planes, members, quarters):
    rows, features = samples.shape
    part = rows // quarters
    return pl.pallas_call(
        pack_kernel,
        in_specs=[IN_SMEM, IN_SMEM, IN_HBM],
        out_specs=IN_HBM,
        out_shape=jax.ShapeDtypeStruct((members, part, features // members), samples.dtype),
        scratch_shapes=[
            pltpu.VMEM((planes, part, features // planes), samples.dtype),
            pltpu.SemaphoreType.DMA((planes,)),
            pltpu.SemaphoreType.DMA((planes * members,)),
        ],
        compiler_params=FULL,
        name="pack",
    )(where, plane, samples)


def three_pieces(value):
    first = value.astype(BF16)
    rest = value - first.astype(F32)
    second = rest.astype(BF16)
    third = (rest - second.astype(F32)).astype(BF16)
    return first, second, third


def prepare_kernel(gram_ref, inverse_ref, expanded_ref, wide_ref):
    rows = gram_ref.shape[0]
    _, size, _ = inverse_ref.shape
    lanes = expanded_ref.shape[3]
    b = pl.program_id(0)
    low = pl.multiple_of(b * size, size)
    high = pl.multiple_of(lax.rem(b + 1, pl.num_programs(0)) * size, size)
    spot = lax.broadcasted_iota(jnp.int32, (rows, size), 0) == low + lax.broadcasted_iota(jnp.int32, (rows, size), 1)
    picks = jnp.where(spot, 1.0, 0.0).astype(BF16)
    sides = [jnp.dot(piece, picks, preferred_element_type=F32) for piece in three_pieces(COUPLING * gram_ref[...])]
    exact = jnp.dot(gram_ref[pl.ds(high, size)], jnp.where(spot, 1.0, 0.0), precision=lax.Precision.HIGHEST, preferred_element_type=F32)
    for k in range(size):
        expanded_ref[0, k] = jnp.broadcast_to(inverse_ref[0, :, k:k + 1], (size, lanes))
        expanded_ref[0, size + k] = COUPLING * jnp.broadcast_to(exact[:, k:k + 1], (size, lanes))
    wide_ref[0] = jnp.concatenate([sides[p].astype(BF16) for p in LEFT], axis=1)


def prepare(gram, inverse, lanes):
    rows = gram.shape[0]
    blocks, size, _ = inverse.shape
    return pl.pallas_call(
        prepare_kernel,
        grid=(blocks,),
        in_specs=[pl.BlockSpec((rows, rows), lambda b: (0, 0)), pl.BlockSpec((1, size, size), lambda b: (b, 0, 0))],
        out_specs=[
            pl.BlockSpec((1, 2 * size, size, lanes), lambda b: (b, 0, 0, 0)),
            pl.BlockSpec((1, rows, len(LEFT) * size), lambda b: (b, 0, 0)),
        ],
        out_shape=[
            jax.ShapeDtypeStruct((blocks, 2 * size, size, lanes), F32),
            jax.ShapeDtypeStruct((blocks, rows, len(LEFT) * size), BF16),
        ],
        compiler_params=FULL,
        name="prepare",
    )(gram, inverse)


def rows_product(expanded, value):
    size = value.shape[0]
    sums = []
    for k in range(size):
        term = expanded[k] * jnp.broadcast_to(value[k:k + 1], value.shape)
        if k < 4:
            sums.append(term)
        else:
            sums[k % 4] += term
    return (sums[0] + sums[1]) + (sums[2] + sums[3])


def passes_kernel(where, start0, start1, start2, start3, labels_hbm, dual_hbm, expanded_hbm, wide_hbm, alpha_hbm, steps_hbm, top_hbm,
                  margin_ref, labels_ref, dual_ref, expanded_ref, wide_ref, alpha_ref, start_ref, sign_ref, change_ref, payload_ref, top_ref, sems):
    rows, width = margin_ref.shape
    blocks = rows // BLOCK
    copies = [
        pltpu.make_async_copy(labels_hbm, labels_ref, sems.at[0]),
        pltpu.make_async_copy(dual_hbm, dual_ref, sems.at[1]),
    ]
    for d, piece in enumerate((start0, start1, start2, start3)):
        part = piece.shape[0]
        low = pl.multiple_of(lax.bitwise_xor(where[0], d) * part, part)
        copies.append(pltpu.make_async_copy(piece, start_ref.at[pl.ds(low, part)], sems.at[2 + d]))
    parts = [
        [pltpu.make_async_copy(expanded_hbm.at[b], expanded_ref.at[b], sems.at[6 + b]),
         pltpu.make_async_copy(wide_hbm.at[b], wide_ref.at[b], sems.at[6 + blocks + b])]
        for b in range(blocks)
    ]
    for copy in copies + [part for pair in parts for part in pair]:
        copy.start()
    change_ref[...] = jnp.zeros((rows, width), F32)
    for copy in copies:
        copy.wait()
    class_ids = where[0] * width + lax.broadcasted_iota(jnp.int32, (rows, width), 1)
    tags = jnp.broadcast_to(labels_ref[...].astype(F32), (width, rows)).T
    sign_ref[...] = jnp.where(tags == class_ids.astype(F32), 1.0, -1.0)
    margin_ref[...] = start_ref[...]
    alpha_ref[...] = dual_ref[...]
    margin = start_ref[:BLOCK]
    for turn in range(PASSES * blocks):
        b = turn % blocks
        at = slice(b * BLOCK, (b + 1) * BLOCK)
        n = (b + 1) % blocks
        if turn < blocks:
            for copy in parts[b]:
                copy.wait()
        signs = sign_ref[at]
        ascent = rows_product(expanded_ref[b, :BLOCK], 1.0 - signs * margin)
        alpha = jnp.clip(alpha_ref[at] + ascent, 0.0, 1.0)
        change = signs * (alpha - dual_ref[at])
        moved = change - change_ref[at]
        alpha_ref[at] = alpha
        change_ref[at] = change
        margin = margin_ref[n * BLOCK:(n + 1) * BLOCK] + rows_product(expanded_ref[b, BLOCK:], moved)
        pieces = three_pieces(moved)
        tall = jnp.concatenate([pieces[p] for p in RIGHT], axis=0)
        margin_ref[...] += jnp.dot(wide_ref[b], tall, preferred_element_type=F32)
    scaled = sign_ref[...] * start_ref[...]
    gap = jnp.sum(jnp.maximum(0.0, 1.0 - scaled) + dual_ref[...] * (scaled - 1.0), axis=0, keepdims=True)
    payload_ref[:rows] = change_ref[...].astype(BF16)
    payload_ref[rows:] = tail_of(gap)
    outs = [pltpu.make_async_copy(payload_ref, steps_hbm.at[place], sems.at[place]) for place in range(steps_hbm.shape[0])]
    for copy in outs:
        copy.start()
    top_ref[...] = jnp.max(margin_ref[...].T, axis=0, keepdims=True)
    after = steps_hbm.shape[0]
    outs += [pltpu.make_async_copy(alpha_ref, alpha_hbm, sems.at[after]), pltpu.make_async_copy(top_ref, top_hbm, sems.at[after + 1])]
    for copy in outs[after:]:
        copy.start()
    for copy in outs:
        copy.wait()


def passes(where, start, labels, dual, ready, members):
    rows, width = dual.shape
    square = pltpu.VMEM((rows, width), F32)
    return pl.pallas_call(
        passes_kernel,
        in_specs=[IN_SMEM] + [IN_HBM] * (len(start) + 4),
        out_specs=[IN_HBM] * 3,
        out_shape=[
            jax.ShapeDtypeStruct((rows, width), F32),
            jax.ShapeDtypeStruct((members, rows + GAP_ROWS, width), BF16),
            jax.ShapeDtypeStruct((1, rows), F32),
        ],
        scratch_shapes=[
            square,
            pltpu.VMEM(labels.shape, labels.dtype),
            square,
            pltpu.VMEM(ready[0].shape, ready[0].dtype),
            pltpu.VMEM(ready[1].shape, ready[1].dtype),
            square,
            square,
            square,
            square,
            pltpu.VMEM((rows + GAP_ROWS, width), BF16),
            pltpu.VMEM((1, rows), F32),
            pltpu.SemaphoreType.DMA((6 + 2 * (rows // BLOCK),)),
        ],
        compiler_params=FULL,
        name="passes",
    )(where, *start, labels, dual, *ready)


def tail_of(gap):
    first, second, third = three_pieces(gap)
    row = lax.broadcasted_iota(jnp.int32, (GAP_ROWS, gap.shape[1]), 0)
    zero = jnp.zeros((GAP_ROWS, gap.shape[1]), F32)
    return jnp.where(row == 0, first.astype(F32), jnp.where(row == 1, second.astype(F32), jnp.where(row == 2, third.astype(F32), zero))).astype(BF16)


def from_tail(tail):
    tail = tail.astype(F32)
    return (tail[0:1] + tail[1:2]) + tail[2:3]


def fetches(held_refs, block_ref, sems, k):
    depth = block_ref.shape[1]
    copies, low = [], 0
    for i, ref in enumerate(held_refs):
        rows = ref.shape[0]
        copies.append(pltpu.make_async_copy(ref.at[:, pl.ds(k * depth, depth)], block_ref.at[pl.ds(low, rows)], sems.at[i]))
        low += rows
    for copy in copies:
        copy.start()
    return copies


def lanes_of(rows):
    return -(-rows // 128) * 128


def product(turned_ref, block_ref, copies, heights):
    total, low, at = None, 0, 0
    for copy, rows in zip(copies, heights):
        copy.wait()
        term = jnp.dot(turned_ref[:, at:at + rows], block_ref[low:low + rows], preferred_element_type=F32)
        total = term if total is None else total + term
        low += rows
        at += lanes_of(rows)
    return total.T


def first_delta_kernel(k, where, *refs):
    *held, steps_ref, sent_ref, turned_ref, gap_ref, block_ref, sems = refs
    copies = fetches(held, block_ref, sems, k)
    members, tall, width = steps_ref.shape
    rows = tall - GAP_ROWS
    part = rows // len(ORDER)
    d, first, at = 0, 0, 0
    for ref in held:
        count = ref.shape[0] // part
        low = pl.multiple_of(lax.bitwise_xor(where[0], d) * part, part)
        picked = jnp.concatenate([steps_ref[g, pl.ds(low, part), :] for g in range(first, first + count)], axis=0)
        turned_ref[:, at:at + count * part] = picked.astype(F32).T.astype(BF16)
        at += lanes_of(count * part)
        d, first = (d + 1, 0) if first + count == members else (d, first + count)
    gap = jnp.zeros((1, width), F32)
    for g in range(members):
        gap += from_tail(steps_ref[g, rows:, :])
    gap_ref[...] = gap
    delta = product(turned_ref, block_ref, copies, [ref.shape[0] for ref in held])
    depth = delta.shape[0]
    sent_ref[:depth] = delta.astype(BF16)
    sent_ref[depth:] = tail_of(gap)


def next_delta_kernel(k, *refs):
    *held, turned_ref, gap_ref, sent_ref, block_ref, sems = refs
    copies = fetches(held, block_ref, sems, k)
    delta = product(turned_ref, block_ref, copies, [ref.shape[0] for ref in held])
    depth = delta.shape[0]
    sent_ref[:depth] = delta.astype(BF16)
    sent_ref[depth:] = tail_of(gap_ref[...])


def own_delta_kernel(*refs):
    *held, turned_ref, sum_ref, block_ref, sems = refs
    copies = fetches(held, block_ref, sems, 0)
    sum_ref[...] = product(turned_ref, block_ref, copies, [ref.shape[0] for ref in held])


def finish_kernel(count, weight_ref, own_ref, gap_ref, *refs):
    *came, new_ref, class_gap_ref = refs
    depth = own_ref.shape[0]
    total, gap = own_ref[...], gap_ref[...]
    for ref in came:
        total += ref[:depth].astype(F32)
        gap += from_tail(ref[depth:])
    new_ref[...] = weight_ref[...].astype(F32) + COUPLING * total
    class_gap_ref[...] = gap / count


def finish(weight, own, gap, came, count):
    depth, width = weight.shape
    whole = pl.BlockSpec(memory_space=pltpu.VMEM)
    return pl.pallas_call(
        functools.partial(finish_kernel, count),
        in_specs=[whole] * (3 + len(came)),
        out_specs=[whole] * 2,
        out_shape=[jax.ShapeDtypeStruct((depth, width), F32), jax.ShapeDtypeStruct((1, width), F32)],
        compiler_params=SMALL,
        name="finish",
    )(weight, own, gap, *came)


def block_scratch(quarters, planes):
    rows = sum(held.shape[0] for held in quarters)
    return [pltpu.VMEM((rows, quarters[0].shape[1] // planes), BF16), pltpu.SemaphoreType.DMA((len(quarters),))]


def first_delta(where, quarters, steps, planes, k):
    features = quarters[0].shape[1]
    width = steps.shape[2]
    return pl.pallas_call(
        functools.partial(first_delta_kernel, k),
        in_specs=[IN_SMEM] + [IN_HBM] * len(quarters) + [IN_VMEM],
        out_specs=[IN_VMEM] * 3,
        out_shape=[
            jax.ShapeDtypeStruct((features // planes + GAP_ROWS, width), BF16),
            jax.ShapeDtypeStruct((width, sum(lanes_of(held.shape[0]) for held in quarters)), BF16),
            jax.ShapeDtypeStruct((1, width), F32),
        ],
        scratch_shapes=block_scratch(quarters, planes),
        compiler_params=SMALL,
        name="delta_first",
    )(where, *quarters, steps)


def next_delta(quarters, turned, gap, planes, k):
    return pl.pallas_call(
        functools.partial(next_delta_kernel, k),
        in_specs=[IN_HBM] * len(quarters) + [IN_VMEM] * 2,
        out_specs=IN_VMEM,
        out_shape=jax.ShapeDtypeStruct((quarters[0].shape[1] // planes + GAP_ROWS, gap.shape[1]), BF16),
        scratch_shapes=block_scratch(quarters, planes),
        compiler_params=SMALL,
        name="delta_next",
    )(*quarters, turned, gap)


def own_delta(quarters, turned, planes):
    return pl.pallas_call(
        own_delta_kernel,
        in_specs=[IN_HBM] * len(quarters) + [IN_VMEM],
        out_specs=IN_VMEM,
        out_shape=jax.ShapeDtypeStruct((quarters[0].shape[1] // planes, turned.shape[0]), F32),
        scratch_shapes=block_scratch(quarters, planes),
        compiler_params=SMALL,
        name="delta_own",
    )(*quarters, turned)


def gathered_kernel(parts_hbm, *refs):
    *outs, parts_ref, sems = refs
    width = outs[0].shape[1]
    copies = [pltpu.make_async_copy(parts_hbm.at[g], parts_ref.at[g], sems.at[g]) for g in range(parts_hbm.shape[0])]
    for copy in copies:
        copy.start()
    copies[0].wait()
    total = parts_ref[0]
    for g in range(1, len(copies)):
        copies[g].wait()
        total += parts_ref[g]
    for i, d in enumerate(ORDER):
        outs[d][...] = total[:, i * width:(i + 1) * width]


def gathered(parts):
    members, part, total = parts.shape
    return pl.pallas_call(
        gathered_kernel,
        in_specs=[IN_HBM],
        out_specs=[IN_VMEM] * len(ORDER),
        out_shape=[jax.ShapeDtypeStruct((part, total // len(ORDER)), F32)] * len(ORDER),
        scratch_shapes=[pltpu.VMEM(parts.shape, F32), pltpu.SemaphoreType.DMA((members,))],
        compiler_params=FULL,
        name="gathered",
    )(parts)


def streamed(rows_hbm, weights_hbm, rows_ref, weights_ref, total_ref, sems, halves):
    chunks, _, depth = rows_ref.shape
    loads, stores = [], []
    for k in range(chunks):
        loads.append(pltpu.make_async_copy(rows_hbm.at[:, pl.ds(k * depth, depth)], rows_ref.at[k], sems.at[2 * k]))
        loads.append(pltpu.make_async_copy(weights_hbm.at[pl.ds(k * depth, depth)], weights_ref.at[k], sems.at[2 * k + 1]))
    for load in loads:
        load.start()
    for k in range(chunks):
        loads[2 * k].wait()
        at = 0
        for h, half in enumerate(halves):
            count = half.shape[0]
            stores.append(pltpu.make_async_copy(
                rows_ref.at[k, pl.ds(at, count)], half.at[:, pl.ds(k * depth, depth)], sems.at[2 * chunks + len(halves) * k + h]
            ))
            stores[-1].start()
            at += count
        loads[2 * k + 1].wait()
        term = jnp.dot(rows_ref[k], weights_ref[k], preferred_element_type=F32)
        if k == 0:
            total_ref[...] = term
        else:
            total_ref[...] += term
    return stores


def first_product_kernel(rows_hbm, weights_hbm, half_hbm, early_hbm, late_hbm, rows_ref, weights_ref, total_ref, sems):
    stores = streamed(rows_hbm, weights_hbm, rows_ref, weights_ref, total_ref, sems, (early_hbm, late_hbm))
    stores.append(pltpu.make_async_copy(total_ref, half_hbm, sems.at[0]))
    stores[-1].start()
    for store in stores:
        store.wait()


def second_product_kernel(rows_hbm, weights_hbm, half_ref, out_hbm, rows_ref, weights_ref, total_ref, sems):
    width = total_ref.shape[1]
    begun = pltpu.make_async_copy(half_ref, out_hbm.at[:, pl.ds(0, width)], sems.at[2 * rows_ref.shape[0]])
    begun.start()
    streamed(rows_hbm, weights_hbm, rows_ref, weights_ref, total_ref, sems, ())
    store = pltpu.make_async_copy(total_ref, out_hbm.at[:, pl.ds(width, width)], sems.at[0])
    store.start()
    store.wait()
    begun.wait()


def product_scratch(rows, weights, chunks):
    depth = rows.shape[1] // chunks
    return [
        pltpu.VMEM((chunks, rows.shape[0], depth), BF16),
        pltpu.VMEM((chunks, depth, weights.shape[1]), BF16),
        pltpu.VMEM((rows.shape[0], weights.shape[1]), F32),
        pltpu.SemaphoreType.DMA((4 * chunks,)),
    ]


def first_product(rows, weights, chunks, early):
    count, features = rows.shape
    return pl.pallas_call(
        first_product_kernel,
        in_specs=[IN_HBM] * 2,
        out_specs=[IN_HBM] * 3,
        out_shape=[
            jax.ShapeDtypeStruct((count, weights.shape[1]), F32),
            jax.ShapeDtypeStruct((early, features), BF16),
            jax.ShapeDtypeStruct((count - early, features), BF16),
        ],
        scratch_shapes=product_scratch(rows, weights, chunks),
        compiler_params=FULL,
        name="product_first",
    )(rows, weights)


def second_product(rows, weights, half, chunks):
    return pl.pallas_call(
        second_product_kernel,
        in_specs=[IN_HBM] * 2 + [IN_VMEM],
        out_specs=IN_HBM,
        out_shape=jax.ShapeDtypeStruct((half.shape[0], 2 * half.shape[1]), F32),
        scratch_shapes=product_scratch(rows, weights, chunks),
        compiler_params=FULL,
        name="product_second",
    )(rows, weights, half)


def self_product(value):
    return lax.dot_general(value, value, (((1,), (1,)), ((), ())), preferred_element_type=F32)


def round_of_ascent(samples, labels, weight, dual, inverse):
    rows = samples.shape[0]
    depth, width = weight.shape
    planes = lax.axis_size(ZH)
    members = lax.axis_size(X) * lax.axis_size(Y)
    quarters = lax.axis_size(ZL) * lax.axis_size(CORE)
    part = rows // quarters
    mine = lax.axis_index(CLS).astype(jnp.int32)
    where = mine.reshape(1)
    plane = lax.axis_index(ZH).astype(jnp.int32).reshape(1)

    packed = pack(samples, where, plane, planes, members, quarters)
    quarter = lax.all_to_all(packed, PLANE, split_axis=0, concat_axis=0, tiled=True)
    from_below = shifted(weight, ZH, 1)
    from_above = shifted(weight, ZH, -1)
    far_head = shifted(from_below[:depth // 2], ZH, 1)
    far_rest = shifted(from_above[depth // 2:], ZH, -1)
    near = [weight, from_below, jnp.concatenate([far_head, far_rest], axis=0), from_above]
    lines = []
    for k in range(planes):
        lines.append(shifted(near[k], ZL, 1))
    by_pair = jnp.concatenate([jnp.concatenate(pair, axis=1) for pair in zip(near, lines)], axis=0)
    by_core_pair = shifted(by_pair, CORE, 1)
    middle = samples.shape[1] // 2
    gram_head = self_product(samples[:, :middle])

    flat = quarter.reshape(members * part, planes * depth)
    early = members * EARLY // 16 * part
    partial, early_rows, late_rows = first_product(flat, by_pair, planes, early)
    beside_a = shifted(early_rows, ZL, 1)
    partial = second_product(flat, by_core_pair, partial, planes)
    partial = lax.all_to_all(partial.reshape(members, part, quarters * width), PLANE, split_axis=0, concat_axis=0, tiled=True)
    across = shifted(flat, CORE, 1)
    diagonal_a = shifted(beside_a, CORE, 1)
    gram = gram_head + self_product(samples[:, middle:])
    ready = prepare(gram, inverse, width)
    own_piece, by_core, by_line, by_both = gathered(partial)
    by_line = shifted(by_line, ZL, 1)
    by_both = lax.ppermute(by_both, CLS, [(i, i ^ 3) for i in range(4)])
    by_core = shifted(by_core, CORE, 1)
    start = [own_piece, by_core, by_line, by_both]
    beside_b = shifted(late_rows, ZL, 1)

    alpha, steps, top = passes(where, start, labels[None, :], dual, ready, members)
    steps = lax.all_to_all(steps, PLANE, split_axis=0, concat_axis=0, tiled=True)
    diagonal_b = shifted(beside_b, CORE, 1)

    top = top[0]
    other = shifted(top, CORE, 1)
    top = jnp.maximum(top, other)
    other = shifted(top, ZL, 1)
    top = jnp.maximum(top, other)

    held = [flat, across, beside_a, beside_b, diagonal_a, diagonal_b]
    far = planes // 2
    sent, turned, gap = first_delta(where, held, steps, planes, far)
    came = [shifted(sent, ZH, planes - far)]
    for k in range(1, planes):
        if k != far:
            sent = next_delta(held, turned, gap, planes, k)
            came.append(shifted(sent, ZH, planes - k))
    own = own_delta(held, turned, planes)
    new_weight, gap = finish(weight, own, gap, came, rows * planes * members)
    return new_weight, alpha, gap[0], top


def solution(mesh):
    fine = Mesh(mesh.devices.reshape(4, 4, 4, 2, 2), (ZH, X, Y, ZL, CORE))
    return jax.shard_map(
        round_of_ascent,
        mesh=fine,
        in_specs=(P(SAMP, None), P(SAMP), P(SAMP, CLS), P(SAMP, CLS), P(SAMP, None, None)),
        out_specs=(P(SAMP, CLS), P(SAMP, CLS), P(CLS), P(SAMP)),
        check_vma=False,
    )
```

```python
import functools

import jax
import jax.numpy as jnp
from jax import lax
from jax.experimental import pallas as pl
from jax.experimental.pallas import tpu as pltpu
from jax.sharding import Mesh, PartitionSpec as P


BLOCK = 16
PASSES = 2
COUPLING = 0.5

ZH, X, Y, ZL, CORE = "zh", "x", "y", "zl", "core"
PLANE = (X, Y)
SAMP = (ZH, X, Y)
CLS = (ZL, CORE)
GAP_ROWS = 8
PACK_PIECES = 4
EARLY = 10
ORDER = (0, 2, 1, 3)
F32, BF16 = jnp.float32, jnp.bfloat16
IN_VMEM = pl.BlockSpec(memory_space=pltpu.VMEM)
IN_SMEM = pl.BlockSpec(memory_space=pltpu.SMEM)
IN_HBM = pl.BlockSpec(memory_space=pltpu.HBM)
LEFT = (0, 0, 1, 1, 0, 2)
RIGHT = (0, 1, 0, 1, 2, 0)
SMALL = pltpu.CompilerParams(vmem_limit_bytes=16 * 2**20)
FULL = pltpu.CompilerParams(vmem_limit_bytes=60 * 1024 * 1024)


def shifted(value, axis, by):
    size = lax.axis_size(axis)
    return lax.ppermute(value, axis, [(i, (i + by) % size) for i in range(size)])


def pack_kernel(where, plane, rows_hbm, out_hbm, held_ref, in_sems, out_sems):
    members, part, total = out_hbm.shape
    planes, pieces = in_sems.shape
    width = total // planes
    span = members * width
    some = members // pieces
    row = pl.multiple_of(where[0] * part, part)
    loads = {}
    for k in range(planes):
        low = pl.multiple_of(lax.rem(plane[0] + (planes - k), planes) * span, span)
        for i in range(pieces):
            loads[k, i] = pltpu.make_async_copy(
                rows_hbm.at[pl.ds(row, part), pl.ds(low + i * some * width, some * width)], held_ref.at[k, i], in_sems.at[k, i]
            )
    for load in loads.values():
        load.start()
    stores = []
    for (k, i), load in loads.items():
        load.wait()
        for place in range(some):
            store = pltpu.make_async_copy(
                held_ref.at[k, i, :, pl.ds(place * width, width)],
                out_hbm.at[i * some + place, :, pl.ds(k * width, width)],
                out_sems.at[k, i * some + place],
            )
            store.start()
            stores.append(store)
    for store in stores:
        store.wait()


def pack(samples, where, plane, planes, members, quarters):
    rows, features = samples.shape
    part = rows // quarters
    return pl.pallas_call(
        pack_kernel,
        in_specs=[IN_SMEM, IN_SMEM, IN_HBM],
        out_specs=IN_HBM,
        out_shape=jax.ShapeDtypeStruct((members, part, features // members), samples.dtype),
        scratch_shapes=[
            pltpu.VMEM((planes, PACK_PIECES, part, features // (planes * PACK_PIECES)), samples.dtype),
            pltpu.SemaphoreType.DMA((planes, PACK_PIECES)),
            pltpu.SemaphoreType.DMA((planes, members)),
        ],
        compiler_params=FULL,
        name="pack",
    )(where, plane, samples)


def three_pieces(value):
    first = value.astype(BF16)
    rest = value - first.astype(F32)
    second = rest.astype(BF16)
    third = (rest - second.astype(F32)).astype(BF16)
    return first, second, third


def prepare_kernel(gram_ref, inverse_ref, expanded_ref, wide_ref):
    rows = gram_ref.shape[0]
    _, size, _ = inverse_ref.shape
    lanes = expanded_ref.shape[3]
    b = pl.program_id(0)
    low = pl.multiple_of(b * size, size)
    high = pl.multiple_of(lax.rem(b + 1, pl.num_programs(0)) * size, size)
    spot = lax.broadcasted_iota(jnp.int32, (rows, size), 0) == low + lax.broadcasted_iota(jnp.int32, (rows, size), 1)
    picks = jnp.where(spot, 1.0, 0.0).astype(BF16)
    sides = [jnp.dot(piece, picks, preferred_element_type=F32) for piece in three_pieces(COUPLING * gram_ref[...])]
    exact = jnp.dot(gram_ref[pl.ds(high, size)], jnp.where(spot, 1.0, 0.0), precision=lax.Precision.HIGHEST, preferred_element_type=F32)
    for k in range(size):
        expanded_ref[0, k] = jnp.broadcast_to(inverse_ref[0, :, k:k + 1], (size, lanes))
        expanded_ref[0, size + k] = COUPLING * jnp.broadcast_to(exact[:, k:k + 1], (size, lanes))
    wide_ref[0] = jnp.concatenate([sides[p].astype(BF16) for p in LEFT], axis=1)


def prepare(gram, inverse, lanes):
    rows = gram.shape[0]
    blocks, size, _ = inverse.shape
    return pl.pallas_call(
        prepare_kernel,
        grid=(blocks,),
        in_specs=[pl.BlockSpec((rows, rows), lambda b: (0, 0)), pl.BlockSpec((1, size, size), lambda b: (b, 0, 0))],
        out_specs=[
            pl.BlockSpec((1, 2 * size, size, lanes), lambda b: (b, 0, 0, 0)),
            pl.BlockSpec((1, rows, len(LEFT) * size), lambda b: (b, 0, 0)),
        ],
        out_shape=[
            jax.ShapeDtypeStruct((blocks, 2 * size, size, lanes), F32),
            jax.ShapeDtypeStruct((blocks, rows, len(LEFT) * size), BF16),
        ],
        compiler_params=FULL,
        name="prepare",
    )(gram, inverse)


def rows_product(expanded, value):
    size = value.shape[0]
    sums = []
    for k in range(size):
        term = expanded[k] * jnp.broadcast_to(value[k:k + 1], value.shape)
        if k < 4:
            sums.append(term)
        else:
            sums[k % 4] += term
    return (sums[0] + sums[1]) + (sums[2] + sums[3])


def passes_kernel(where, start0, start1, start2, start3, labels_hbm, dual_hbm, expanded_hbm, wide_hbm, alpha_hbm, steps_hbm, top_hbm,
                  margin_ref, labels_ref, dual_ref, expanded_ref, wide_ref, alpha_ref, start_ref, sign_ref, change_ref, payload_ref, top_ref, sems):
    rows, width = margin_ref.shape
    blocks = rows // BLOCK
    copies = [
        pltpu.make_async_copy(labels_hbm, labels_ref, sems.at[0]),
        pltpu.make_async_copy(dual_hbm, dual_ref, sems.at[1]),
    ]
    for d, piece in enumerate((start0, start1, start2, start3)):
        part = piece.shape[0]
        low = pl.multiple_of(lax.bitwise_xor(where[0], d) * part, part)
        copies.append(pltpu.make_async_copy(piece, start_ref.at[pl.ds(low, part)], sems.at[2 + d]))
    parts = [
        [pltpu.make_async_copy(expanded_hbm.at[b], expanded_ref.at[b], sems.at[6 + b]),
         pltpu.make_async_copy(wide_hbm.at[b], wide_ref.at[b], sems.at[6 + blocks + b])]
        for b in range(blocks)
    ]
    for copy in copies + [part for pair in parts for part in pair]:
        copy.start()
    change_ref[...] = jnp.zeros((rows, width), F32)
    for copy in copies:
        copy.wait()
    class_ids = where[0] * width + lax.broadcasted_iota(jnp.int32, (rows, width), 1)
    tags = jnp.broadcast_to(labels_ref[...].astype(F32), (width, rows)).T
    sign_ref[...] = jnp.where(tags == class_ids.astype(F32), 1.0, -1.0)
    margin_ref[...] = start_ref[...]
    alpha_ref[...] = dual_ref[...]
    margin = start_ref[:BLOCK]
    for turn in range(PASSES * blocks):
        b = turn % blocks
        at = slice(b * BLOCK, (b + 1) * BLOCK)
        n = (b + 1) % blocks
        if turn < blocks:
            for copy in parts[b]:
                copy.wait()
        signs = sign_ref[at]
        ascent = rows_product(expanded_ref[b, :BLOCK], 1.0 - signs * margin)
        alpha = jnp.clip(alpha_ref[at] + ascent, 0.0, 1.0)
        change = signs * (alpha - dual_ref[at])
        moved = change - change_ref[at]
        alpha_ref[at] = alpha
        change_ref[at] = change
        margin = margin_ref[n * BLOCK:(n + 1) * BLOCK] + rows_product(expanded_ref[b, BLOCK:], moved)
        pieces = three_pieces(moved)
        tall = jnp.concatenate([pieces[p] for p in RIGHT], axis=0)
        margin_ref[...] += jnp.dot(wide_ref[b], tall, preferred_element_type=F32)
    scaled = sign_ref[...] * start_ref[...]
    gap = jnp.sum(jnp.maximum(0.0, 1.0 - scaled) + dual_ref[...] * (scaled - 1.0), axis=0, keepdims=True)
    payload_ref[:rows] = change_ref[...].astype(BF16)
    payload_ref[rows:] = tail_of(gap)
    outs = [pltpu.make_async_copy(payload_ref, steps_hbm.at[place], sems.at[place]) for place in range(steps_hbm.shape[0])]
    for copy in outs:
        copy.start()
    top_ref[...] = jnp.max(margin_ref[...].T, axis=0, keepdims=True)
    after = steps_hbm.shape[0]
    outs += [pltpu.make_async_copy(alpha_ref, alpha_hbm, sems.at[after]), pltpu.make_async_copy(top_ref, top_hbm, sems.at[after + 1])]
    for copy in outs[after:]:
        copy.start()
    for copy in outs:
        copy.wait()


def passes(where, start, labels, dual, ready, members):
    rows, width = dual.shape
    square = pltpu.VMEM((rows, width), F32)
    return pl.pallas_call(
        passes_kernel,
        in_specs=[IN_SMEM] + [IN_HBM] * (len(start) + 4),
        out_specs=[IN_HBM] * 3,
        out_shape=[
            jax.ShapeDtypeStruct((rows, width), F32),
            jax.ShapeDtypeStruct((members, rows + GAP_ROWS, width), BF16),
            jax.ShapeDtypeStruct((1, rows), F32),
        ],
        scratch_shapes=[
            square,
            pltpu.VMEM(labels.shape, labels.dtype),
            square,
            pltpu.VMEM(ready[0].shape, ready[0].dtype),
            pltpu.VMEM(ready[1].shape, ready[1].dtype),
            square,
            square,
            square,
            square,
            pltpu.VMEM((rows + GAP_ROWS, width), BF16),
            pltpu.VMEM((1, rows), F32),
            pltpu.SemaphoreType.DMA((6 + 2 * (rows // BLOCK),)),
        ],
        compiler_params=FULL,
        name="passes",
    )(where, *start, labels, dual, *ready)


def tail_of(gap):
    first, second, third = three_pieces(gap)
    row = lax.broadcasted_iota(jnp.int32, (GAP_ROWS, gap.shape[1]), 0)
    zero = jnp.zeros((GAP_ROWS, gap.shape[1]), F32)
    return jnp.where(row == 0, first.astype(F32), jnp.where(row == 1, second.astype(F32), jnp.where(row == 2, third.astype(F32), zero))).astype(BF16)


def from_tail(tail):
    tail = tail.astype(F32)
    return (tail[0:1] + tail[1:2]) + tail[2:3]


def fetches(held_refs, block_ref, sems, k):
    depth = block_ref.shape[1]
    copies, low = [], 0
    for i, ref in enumerate(held_refs):
        rows = ref.shape[0]
        copies.append(pltpu.make_async_copy(ref.at[:, pl.ds(k * depth, depth)], block_ref.at[pl.ds(low, rows)], sems.at[i]))
        low += rows
    for copy in copies:
        copy.start()
    return copies


def lanes_of(rows):
    return -(-rows // 128) * 128


def product(turned_ref, block_ref, copies, heights):
    total, low, at = None, 0, 0
    for copy, rows in zip(copies, heights):
        copy.wait()
        term = jnp.dot(turned_ref[:, at:at + rows], block_ref[low:low + rows], preferred_element_type=F32)
        total = term if total is None else total + term
        low += rows
        at += lanes_of(rows)
    return total.T


def first_delta_kernel(k, where, *refs):
    *held, steps_ref, sent_ref, turned_ref, gap_ref, block_ref, sems = refs
    copies = fetches(held, block_ref, sems, k)
    members, tall, width = steps_ref.shape
    rows = tall - GAP_ROWS
    part = rows // len(ORDER)
    d, first, at = 0, 0, 0
    for ref in held:
        count = ref.shape[0] // part
        low = pl.multiple_of(lax.bitwise_xor(where[0], d) * part, part)
        picked = jnp.concatenate([steps_ref[g, pl.ds(low, part), :] for g in range(first, first + count)], axis=0)
        turned_ref[:, at:at + count * part] = picked.astype(F32).T.astype(BF16)
        at += lanes_of(count * part)
        d, first = (d + 1, 0) if first + count == members else (d, first + count)
    gap = jnp.zeros((1, width), F32)
    for g in range(members):
        gap += from_tail(steps_ref[g, rows:, :])
    gap_ref[...] = gap
    delta = product(turned_ref, block_ref, copies, [ref.shape[0] for ref in held])
    depth = delta.shape[0]
    sent_ref[:depth] = delta.astype(BF16)
    sent_ref[depth:] = tail_of(gap)


def next_delta_kernel(k, *refs):
    *held, turned_ref, gap_ref, sent_ref, block_ref, sems = refs
    copies = fetches(held, block_ref, sems, k)
    delta = product(turned_ref, block_ref, copies, [ref.shape[0] for ref in held])
    depth = delta.shape[0]
    sent_ref[:depth] = delta.astype(BF16)
    sent_ref[depth:] = tail_of(gap_ref[...])


def own_delta_kernel(*refs):
    *held, turned_ref, sum_ref, block_ref, sems = refs
    copies = fetches(held, block_ref, sems, 0)
    sum_ref[...] = product(turned_ref, block_ref, copies, [ref.shape[0] for ref in held])


def finish_kernel(count, weight_ref, own_ref, gap_ref, *refs):
    *came, new_ref, class_gap_ref = refs
    depth = own_ref.shape[0]
    total, gap = own_ref[...], gap_ref[...]
    for ref in came:
        total += ref[:depth].astype(F32)
        gap += from_tail(ref[depth:])
    new_ref[...] = weight_ref[...].astype(F32) + COUPLING * total
    class_gap_ref[...] = gap / count


def finish(weight, own, gap, came, count):
    depth, width = weight.shape
    whole = pl.BlockSpec(memory_space=pltpu.VMEM)
    return pl.pallas_call(
        functools.partial(finish_kernel, count),
        in_specs=[whole] * (3 + len(came)),
        out_specs=[whole] * 2,
        out_shape=[jax.ShapeDtypeStruct((depth, width), F32), jax.ShapeDtypeStruct((1, width), F32)],
        compiler_params=SMALL,
        name="finish",
    )(weight, own, gap, *came)


def block_scratch(quarters, planes):
    rows = sum(held.shape[0] for held in quarters)
    return [pltpu.VMEM((rows, quarters[0].shape[1] // planes), BF16), pltpu.SemaphoreType.DMA((len(quarters),))]


def first_delta(where, quarters, steps, planes, k):
    features = quarters[0].shape[1]
    width = steps.shape[2]
    return pl.pallas_call(
        functools.partial(first_delta_kernel, k),
        in_specs=[IN_SMEM] + [IN_HBM] * len(quarters) + [IN_VMEM],
        out_specs=[IN_VMEM] * 3,
        out_shape=[
            jax.ShapeDtypeStruct((features // planes + GAP_ROWS, width), BF16),
            jax.ShapeDtypeStruct((width, sum(lanes_of(held.shape[0]) for held in quarters)), BF16),
            jax.ShapeDtypeStruct((1, width), F32),
        ],
        scratch_shapes=block_scratch(quarters, planes),
        compiler_params=SMALL,
        name="delta_first",
    )(where, *quarters, steps)


def next_delta(quarters, turned, gap, planes, k):
    return pl.pallas_call(
        functools.partial(next_delta_kernel, k),
        in_specs=[IN_HBM] * len(quarters) + [IN_VMEM] * 2,
        out_specs=IN_VMEM,
        out_shape=jax.ShapeDtypeStruct((quarters[0].shape[1] // planes + GAP_ROWS, gap.shape[1]), BF16),
        scratch_shapes=block_scratch(quarters, planes),
        compiler_params=SMALL,
        name="delta_next",
    )(*quarters, turned, gap)


def own_delta(quarters, turned, planes):
    return pl.pallas_call(
        own_delta_kernel,
        in_specs=[IN_HBM] * len(quarters) + [IN_VMEM],
        out_specs=IN_VMEM,
        out_shape=jax.ShapeDtypeStruct((quarters[0].shape[1] // planes, turned.shape[0]), F32),
        scratch_shapes=block_scratch(quarters, planes),
        compiler_params=SMALL,
        name="delta_own",
    )(*quarters, turned)


def gathered_kernel(parts_hbm, *refs):
    *outs, parts_ref, sems = refs
    width = outs[0].shape[1]
    copies = [pltpu.make_async_copy(parts_hbm.at[g], parts_ref.at[g], sems.at[g]) for g in range(parts_hbm.shape[0])]
    for copy in copies:
        copy.start()
    copies[0].wait()
    total = parts_ref[0]
    for g in range(1, len(copies)):
        copies[g].wait()
        total += parts_ref[g]
    for i, d in enumerate(ORDER):
        outs[d][...] = total[:, i * width:(i + 1) * width]


def gathered(parts):
    members, part, total = parts.shape
    return pl.pallas_call(
        gathered_kernel,
        in_specs=[IN_HBM],
        out_specs=[IN_VMEM] * len(ORDER),
        out_shape=[jax.ShapeDtypeStruct((part, total // len(ORDER)), F32)] * len(ORDER),
        scratch_shapes=[pltpu.VMEM(parts.shape, F32), pltpu.SemaphoreType.DMA((members,))],
        compiler_params=FULL,
        name="gathered",
    )(parts)


def self_product(value):
    return lax.dot_general(value, value, (((1,), (1,)), ((), ())), preferred_element_type=F32)


def round_of_ascent(samples, labels, weight, dual, inverse):
    rows = samples.shape[0]
    depth, width = weight.shape
    planes = lax.axis_size(ZH)
    members = lax.axis_size(X) * lax.axis_size(Y)
    quarters = lax.axis_size(ZL) * lax.axis_size(CORE)
    part = rows // quarters
    mine = lax.axis_index(CLS).astype(jnp.int32)
    where = mine.reshape(1)
    plane = lax.axis_index(ZH).astype(jnp.int32).reshape(1)

    packed = pack(samples, where, plane, planes, members, quarters)
    quarter = lax.all_to_all(packed, PLANE, split_axis=0, concat_axis=0, tiled=True)
    from_below = shifted(weight, ZH, 1)
    from_above = shifted(weight, ZH, -1)
    far_head = shifted(from_below[:depth // 2], ZH, 1)
    far_rest = shifted(from_above[depth // 2:], ZH, -1)
    near = {"0": weight, "1": from_below, "2_head": far_head, "2_rest": far_rest, "3": from_above}
    pairs = []
    for piece in near.values():
        other = shifted(piece, ZL, 1)
        pairs.append(jnp.concatenate([piece, other], axis=1))
    by_pair = jnp.concatenate(pairs, axis=0)
    by_all = jnp.concatenate([by_pair, shifted(by_pair, CORE, 1)], axis=1)
    middle = samples.shape[1] // 2
    gram_head = self_product(samples[:, :middle])

    flat = quarter.reshape(members * part, planes * depth)
    early = members * EARLY // 16 * part
    beside_a = shifted(flat[:early], ZL, 1)
    partial = jnp.dot(flat, by_all, preferred_element_type=F32)
    partial, late = lax.optimization_barrier((partial, flat))
    partial = lax.all_to_all(partial.reshape(members, part, quarters * width), PLANE, split_axis=0, concat_axis=0, tiled=True)
    across = shifted(flat, CORE, 1)
    diagonal_a = shifted(beside_a, CORE, 1)
    gram = gram_head + self_product(samples[:, middle:])
    ready = prepare(gram, inverse, width)
    partial, late = lax.optimization_barrier((partial, late[early:]))
    own_piece, by_core, by_line, by_both = gathered(partial)
    by_line = shifted(by_line, ZL, 1)
    by_both = lax.ppermute(by_both, CLS, [(i, i ^ 3) for i in range(4)])
    by_core = shifted(by_core, CORE, 1)
    start = [own_piece, by_core, by_line, by_both]
    beside_b = shifted(late, ZL, 1)

    alpha, steps, top = passes(where, start, labels[None, :], dual, ready, members)
    steps = lax.all_to_all(steps, PLANE, split_axis=0, concat_axis=0, tiled=True)
    diagonal_b = shifted(beside_b, CORE, 1)

    top = top[0]
    other = shifted(top, CORE, 1)
    top = jnp.maximum(top, other)
    other = shifted(top, ZL, 1)
    top = jnp.maximum(top, other)

    held = [flat, across, beside_a, beside_b, diagonal_a, diagonal_b]
    far = planes // 2
    sent, turned, gap = first_delta(where, held, steps, planes, far)
    came = [shifted(sent, ZH, planes - far)]
    for k in range(1, planes):
        if k != far:
            sent = next_delta(held, turned, gap, planes, k)
            came.append(shifted(sent, ZH, planes - k))
    own = own_delta(held, turned, planes)
    new_weight, gap = finish(weight, own, gap, came, rows * planes * members)
    return new_weight, alpha, gap[0], top


def solution(mesh):
    fine = Mesh(mesh.devices.reshape(4, 4, 4, 2, 2), (ZH, X, Y, ZL, CORE))
    return jax.shard_map(
        round_of_ascent,
        mesh=fine,
        in_specs=(P(SAMP, None), P(SAMP), P(SAMP, CLS), P(SAMP, CLS), P(SAMP, None, None)),
        out_specs=(P(SAMP, CLS), P(SAMP, CLS), P(CLS), P(SAMP)),
        check_vma=False,
    )
```

```python
import functools

import jax
import jax.numpy as jnp
from jax import lax
from jax.experimental import pallas as pl
from jax.experimental.pallas import tpu as pltpu
from jax.sharding import Mesh, PartitionSpec as P


BLOCK = 16
PASSES = 2
COUPLING = 0.5

ZH, X, Y, ZL, CORE = "zh", "x", "y", "zl", "core"
PLANE = (X, Y)
SAMP = (ZH, X, Y)
CLS = (ZL, CORE)
GAP_ROWS = 8
PACK_PIECES = 4
EARLY = 10
ORDER = (0, 2, 1, 3)
F32, BF16 = jnp.float32, jnp.bfloat16
IN_VMEM = pl.BlockSpec(memory_space=pltpu.VMEM)
IN_SMEM = pl.BlockSpec(memory_space=pltpu.SMEM)
IN_HBM = pl.BlockSpec(memory_space=pltpu.HBM)
LEFT = (0, 0, 1, 1, 0, 2)
RIGHT = (0, 1, 0, 1, 2, 0)
SMALL = pltpu.CompilerParams(vmem_limit_bytes=16 * 2**20)
FULL = pltpu.CompilerParams(vmem_limit_bytes=60 * 1024 * 1024)


def shifted(value, axis, by):
    size = lax.axis_size(axis)
    return lax.ppermute(value, axis, [(i, (i + by) % size) for i in range(size)])


def pack_kernel(where, plane, rows_hbm, out_hbm, held_ref, in_sems, out_sems):
    members, part, total = out_hbm.shape
    planes, pieces = in_sems.shape
    width = total // planes
    span = members * width
    some = members // pieces
    row = pl.multiple_of(where[0] * part, part)
    loads = {}
    for k in range(planes):
        low = pl.multiple_of(lax.rem(plane[0] + (planes - k), planes) * span, span)
        for i in range(pieces):
            loads[k, i] = pltpu.make_async_copy(
                rows_hbm.at[pl.ds(row, part), pl.ds(low + i * some * width, some * width)], held_ref.at[k, i], in_sems.at[k, i]
            )
    for load in loads.values():
        load.start()
    stores = []
    for (k, i), load in loads.items():
        load.wait()
        for place in range(some):
            store = pltpu.make_async_copy(
                held_ref.at[k, i, :, pl.ds(place * width, width)],
                out_hbm.at[i * some + place, :, pl.ds(k * width, width)],
                out_sems.at[k, i * some + place],
            )
            store.start()
            stores.append(store)
    for store in stores:
        store.wait()


def pack(samples, where, plane, planes, members, quarters):
    rows, features = samples.shape
    part = rows // quarters
    return pl.pallas_call(
        pack_kernel,
        in_specs=[IN_SMEM, IN_SMEM, IN_HBM],
        out_specs=IN_HBM,
        out_shape=jax.ShapeDtypeStruct((members, part, features // members), samples.dtype),
        scratch_shapes=[
            pltpu.VMEM((planes, PACK_PIECES, part, features // (planes * PACK_PIECES)), samples.dtype),
            pltpu.SemaphoreType.DMA((planes, PACK_PIECES)),
            pltpu.SemaphoreType.DMA((planes, members)),
        ],
        compiler_params=FULL,
        name="pack",
    )(where, plane, samples)


def three_pieces(value):
    first = value.astype(BF16)
    rest = value - first.astype(F32)
    second = rest.astype(BF16)
    third = (rest - second.astype(F32)).astype(BF16)
    return first, second, third


def prepare_kernel(gram_ref, inverse_ref, expanded_ref, wide_ref, columns_ref):
    rows = gram_ref.shape[0]
    count, size, _ = inverse_ref.shape
    lanes = expanded_ref.shape[3]
    blocks = rows // size
    pieces = three_pieces(COUPLING * gram_ref[...])
    for i in range(count):
        b = pl.program_id(0) * count + i
        low = pl.multiple_of(b * size, size)
        high = pl.multiple_of(lax.rem(b + 1, blocks) * size, size)
        spot = lax.broadcasted_iota(jnp.int32, (rows, size), 0) == low + lax.broadcasted_iota(jnp.int32, (rows, size), 1)
        picks = jnp.where(spot, 1.0, 0.0).astype(BF16)
        sides = [jnp.dot(piece, picks, preferred_element_type=F32) for piece in pieces]
        columns_ref[i] = (sides[0] + sides[1]) + sides[2]
        ahead = columns_ref[i, pl.ds(high, size)]
        for k in range(size):
            expanded_ref[i, k] = jnp.broadcast_to(inverse_ref[i, :, k:k + 1], (size, lanes))
            expanded_ref[i, size + k] = jnp.broadcast_to(ahead[:, k:k + 1], (size, lanes))
        wide_ref[i] = jnp.concatenate([sides[p].astype(BF16) for p in LEFT], axis=1)


def prepare(gram, inverse, lanes):
    rows = gram.shape[0]
    blocks, size, _ = inverse.shape
    some = 2
    return pl.pallas_call(
        prepare_kernel,
        grid=(blocks // some,),
        in_specs=[pl.BlockSpec((rows, rows), lambda b: (0, 0)), pl.BlockSpec((some, size, size), lambda b: (b, 0, 0))],
        out_specs=[
            pl.BlockSpec((some, 2 * size, size, lanes), lambda b: (b, 0, 0, 0)),
            pl.BlockSpec((some, rows, len(LEFT) * size), lambda b: (b, 0, 0)),
        ],
        out_shape=[
            jax.ShapeDtypeStruct((blocks, 2 * size, size, lanes), F32),
            jax.ShapeDtypeStruct((blocks, rows, len(LEFT) * size), BF16),
        ],
        scratch_shapes=[pltpu.VMEM((some, rows, size), F32)],
        compiler_params=FULL,
        name="prepare",
    )(gram, inverse)


def rows_product(expanded, value):
    size = value.shape[0]
    sums = []
    for k in range(size):
        term = expanded[k] * jnp.broadcast_to(value[k:k + 1], value.shape)
        if k < 4:
            sums.append(term)
        else:
            sums[k % 4] += term
    return (sums[0] + sums[1]) + (sums[2] + sums[3])


def passes_kernel(where, start0, start1, start2, start3, labels_hbm, dual_hbm, expanded_hbm, wide_hbm, alpha_hbm, steps_hbm, top_hbm,
                  margin_ref, labels_ref, dual_ref, expanded_ref, wide_ref, alpha_ref, start_ref, sign_ref, change_ref, payload_ref, top_ref, sems):
    rows, width = margin_ref.shape
    blocks = rows // BLOCK
    copies = [
        pltpu.make_async_copy(labels_hbm, labels_ref, sems.at[0]),
        pltpu.make_async_copy(dual_hbm, dual_ref, sems.at[1]),
    ]
    for d, piece in enumerate((start0, start1, start2, start3)):
        part = piece.shape[0]
        low = pl.multiple_of(lax.bitwise_xor(where[0], d) * part, part)
        copies.append(pltpu.make_async_copy(piece, start_ref.at[pl.ds(low, part)], sems.at[2 + d]))
    parts = [
        [pltpu.make_async_copy(expanded_hbm.at[b], expanded_ref.at[b], sems.at[6 + b]),
         pltpu.make_async_copy(wide_hbm.at[b], wide_ref.at[b], sems.at[6 + blocks + b])]
        for b in range(blocks)
    ]
    for copy in copies + [part for pair in parts for part in pair]:
        copy.start()
    change_ref[...] = jnp.zeros((rows, width), F32)
    for copy in copies:
        copy.wait()
    class_ids = where[0] * width + lax.broadcasted_iota(jnp.int32, (rows, width), 1)
    tags = jnp.broadcast_to(labels_ref[...].astype(F32), (width, rows)).T
    sign_ref[...] = jnp.where(tags == class_ids.astype(F32), 1.0, -1.0)
    margin_ref[...] = start_ref[...]
    alpha_ref[...] = dual_ref[...]
    margin = start_ref[:BLOCK]
    for turn in range(PASSES * blocks):
        b = turn % blocks
        at = slice(b * BLOCK, (b + 1) * BLOCK)
        n = (b + 1) % blocks
        if turn < blocks:
            for copy in parts[b]:
                copy.wait()
        signs = sign_ref[at]
        ascent = rows_product(expanded_ref[b, :BLOCK], 1.0 - signs * margin)
        alpha = jnp.clip(alpha_ref[at] + ascent, 0.0, 1.0)
        change = signs * (alpha - dual_ref[at])
        moved = change - change_ref[at]
        alpha_ref[at] = alpha
        change_ref[at] = change
        margin = margin_ref[n * BLOCK:(n + 1) * BLOCK] + rows_product(expanded_ref[b, BLOCK:], moved)
        pieces = three_pieces(moved)
        tall = jnp.concatenate([pieces[p] for p in RIGHT], axis=0)
        margin_ref[...] += jnp.dot(wide_ref[b], tall, preferred_element_type=F32)
    scaled = sign_ref[...] * start_ref[...]
    gap = jnp.sum(jnp.maximum(0.0, 1.0 - scaled) + dual_ref[...] * (scaled - 1.0), axis=0, keepdims=True)
    payload_ref[:rows] = change_ref[...].astype(BF16)
    payload_ref[rows:] = tail_of(gap)
    outs = [pltpu.make_async_copy(payload_ref, steps_hbm.at[place], sems.at[place]) for place in range(steps_hbm.shape[0])]
    for copy in outs:
        copy.start()
    top_ref[...] = jnp.max(margin_ref[...].T, axis=0, keepdims=True)
    after = steps_hbm.shape[0]
    outs += [pltpu.make_async_copy(alpha_ref, alpha_hbm, sems.at[after]), pltpu.make_async_copy(top_ref, top_hbm, sems.at[after + 1])]
    for copy in outs[after:]:
        copy.start()
    for copy in outs:
        copy.wait()


def passes(where, start, labels, dual, ready, members):
    rows, width = dual.shape
    square = pltpu.VMEM((rows, width), F32)
    return pl.pallas_call(
        passes_kernel,
        in_specs=[IN_SMEM] + [IN_HBM] * (len(start) + 4),
        out_specs=[IN_HBM] * 3,
        out_shape=[
            jax.ShapeDtypeStruct((rows, width), F32),
            jax.ShapeDtypeStruct((members, rows + GAP_ROWS, width), BF16),
            jax.ShapeDtypeStruct((1, rows), F32),
        ],
        scratch_shapes=[
            square,
            pltpu.VMEM(labels.shape, labels.dtype),
            square,
            pltpu.VMEM(ready[0].shape, ready[0].dtype),
            pltpu.VMEM(ready[1].shape, ready[1].dtype),
            square,
            square,
            square,
            square,
            pltpu.VMEM((rows + GAP_ROWS, width), BF16),
            pltpu.VMEM((1, rows), F32),
            pltpu.SemaphoreType.DMA((6 + 2 * (rows // BLOCK),)),
        ],
        compiler_params=FULL,
        name="passes",
    )(where, *start, labels, dual, *ready)


def tail_of(gap):
    first, second, third = three_pieces(gap)
    row = lax.broadcasted_iota(jnp.int32, (GAP_ROWS, gap.shape[1]), 0)
    zero = jnp.zeros((GAP_ROWS, gap.shape[1]), F32)
    return jnp.where(row == 0, first.astype(F32), jnp.where(row == 1, second.astype(F32), jnp.where(row == 2, third.astype(F32), zero))).astype(BF16)


def from_tail(tail):
    tail = tail.astype(F32)
    return (tail[0:1] + tail[1:2]) + tail[2:3]


def fetches(held_refs, block_ref, sems, k):
    depth = block_ref.shape[1]
    copies, low = [], 0
    for i, ref in enumerate(held_refs):
        rows = ref.shape[0]
        copies.append(pltpu.make_async_copy(ref.at[:, pl.ds(k * depth, depth)], block_ref.at[pl.ds(low, rows)], sems.at[i]))
        low += rows
    for copy in copies:
        copy.start()
    return copies


def lanes_of(rows):
    return -(-rows // 128) * 128


def product(turned_ref, block_ref, copies, heights):
    total, low, at = None, 0, 0
    for copy, rows in zip(copies, heights):
        copy.wait()
        term = jnp.dot(turned_ref[:, at:at + rows], block_ref[low:low + rows], preferred_element_type=F32)
        total = term if total is None else total + term
        low += rows
        at += lanes_of(rows)
    return total.T


def first_delta_kernel(k, where, *refs):
    *held, steps_ref, sent_ref, turned_ref, gap_ref, block_ref, sems = refs
    copies = fetches(held, block_ref, sems, k)
    members, tall, width = steps_ref.shape
    rows = tall - GAP_ROWS
    part = rows // len(ORDER)
    d, first, at = 0, 0, 0
    for ref in held:
        count = ref.shape[0] // part
        low = pl.multiple_of(lax.bitwise_xor(where[0], d) * part, part)
        picked = jnp.concatenate([steps_ref[g, pl.ds(low, part), :] for g in range(first, first + count)], axis=0)
        turned_ref[:, at:at + count * part] = picked.astype(F32).T.astype(BF16)
        at += lanes_of(count * part)
        d, first = (d + 1, 0) if first + count == members else (d, first + count)
    gap = jnp.zeros((1, width), F32)
    for g in range(members):
        gap += from_tail(steps_ref[g, rows:, :])
    gap_ref[...] = gap
    delta = product(turned_ref, block_ref, copies, [ref.shape[0] for ref in held])
    depth = delta.shape[0]
    sent_ref[:depth] = delta.astype(BF16)
    sent_ref[depth:] = tail_of(gap)


def next_delta_kernel(k, *refs):
    *held, turned_ref, gap_ref, sent_ref, block_ref, sems = refs
    copies = fetches(held, block_ref, sems, k)
    delta = product(turned_ref, block_ref, copies, [ref.shape[0] for ref in held])
    depth = delta.shape[0]
    sent_ref[:depth] = delta.astype(BF16)
    sent_ref[depth:] = tail_of(gap_ref[...])


def own_delta_kernel(*refs):
    *held, turned_ref, sum_ref, block_ref, sems = refs
    copies = fetches(held, block_ref, sems, 0)
    sum_ref[...] = product(turned_ref, block_ref, copies, [ref.shape[0] for ref in held])


def finish_kernel(count, weight_ref, own_ref, gap_ref, *refs):
    *came, new_ref, class_gap_ref = refs
    depth = own_ref.shape[0]
    total, gap = own_ref[...], gap_ref[...]
    for ref in came:
        total += ref[:depth].astype(F32)
        gap += from_tail(ref[depth:])
    new_ref[...] = weight_ref[...].astype(F32) + COUPLING * total
    class_gap_ref[...] = gap / count


def finish(weight, own, gap, came, count):
    depth, width = weight.shape
    whole = pl.BlockSpec(memory_space=pltpu.VMEM)
    return pl.pallas_call(
        functools.partial(finish_kernel, count),
        in_specs=[whole] * (3 + len(came)),
        out_specs=[whole] * 2,
        out_shape=[jax.ShapeDtypeStruct((depth, width), F32), jax.ShapeDtypeStruct((1, width), F32)],
        compiler_params=SMALL,
        name="finish",
    )(weight, own, gap, *came)


def block_scratch(quarters, planes):
    rows = sum(held.shape[0] for held in quarters)
    return [pltpu.VMEM((rows, quarters[0].shape[1] // planes), BF16), pltpu.SemaphoreType.DMA((len(quarters),))]


def first_delta(where, quarters, steps, planes, k):
    features = quarters[0].shape[1]
    width = steps.shape[2]
    return pl.pallas_call(
        functools.partial(first_delta_kernel, k),
        in_specs=[IN_SMEM] + [IN_HBM] * len(quarters) + [IN_VMEM],
        out_specs=[IN_VMEM] * 3,
        out_shape=[
            jax.ShapeDtypeStruct((features // planes + GAP_ROWS, width), BF16),
            jax.ShapeDtypeStruct((width, sum(lanes_of(held.shape[0]) for held in quarters)), BF16),
            jax.ShapeDtypeStruct((1, width), F32),
        ],
        scratch_shapes=block_scratch(quarters, planes),
        compiler_params=SMALL,
        name="delta_first",
    )(where, *quarters, steps)


def next_delta(quarters, turned, gap, planes, k):
    return pl.pallas_call(
        functools.partial(next_delta_kernel, k),
        in_specs=[IN_HBM] * len(quarters) + [IN_VMEM] * 2,
        out_specs=IN_VMEM,
        out_shape=jax.ShapeDtypeStruct((quarters[0].shape[1] // planes + GAP_ROWS, gap.shape[1]), BF16),
        scratch_shapes=block_scratch(quarters, planes),
        compiler_params=SMALL,
        name="delta_next",
    )(*quarters, turned, gap)


def own_delta(quarters, turned, planes):
    return pl.pallas_call(
        own_delta_kernel,
        in_specs=[IN_HBM] * len(quarters) + [IN_VMEM],
        out_specs=IN_VMEM,
        out_shape=jax.ShapeDtypeStruct((quarters[0].shape[1] // planes, turned.shape[0]), F32),
        scratch_shapes=block_scratch(quarters, planes),
        compiler_params=SMALL,
        name="delta_own",
    )(*quarters, turned)


def gathered_kernel(parts_hbm, *refs):
    *outs, parts_ref, sems = refs
    width = outs[0].shape[1]
    copies = [pltpu.make_async_copy(parts_hbm.at[g], parts_ref.at[g], sems.at[g]) for g in range(parts_hbm.shape[0])]
    for copy in copies:
        copy.start()
    copies[0].wait()
    total = parts_ref[0]
    for g in range(1, len(copies)):
        copies[g].wait()
        total += parts_ref[g]
    for i, d in enumerate(ORDER):
        outs[d][...] = total[:, i * width:(i + 1) * width]


def gathered(parts):
    members, part, total = parts.shape
    return pl.pallas_call(
        gathered_kernel,
        in_specs=[IN_HBM],
        out_specs=[IN_VMEM] * len(ORDER),
        out_shape=[jax.ShapeDtypeStruct((part, total // len(ORDER)), F32)] * len(ORDER),
        scratch_shapes=[pltpu.VMEM(parts.shape, F32), pltpu.SemaphoreType.DMA((members,))],
        compiler_params=FULL,
        name="gathered",
    )(parts)


def self_product(value):
    return lax.dot_general(value, value, (((1,), (1,)), ((), ())), preferred_element_type=F32)


def round_of_ascent(samples, labels, weight, dual, inverse):
    rows = samples.shape[0]
    depth, width = weight.shape
    planes = lax.axis_size(ZH)
    members = lax.axis_size(X) * lax.axis_size(Y)
    quarters = lax.axis_size(ZL) * lax.axis_size(CORE)
    part = rows // quarters
    mine = lax.axis_index(CLS).astype(jnp.int32)
    where = mine.reshape(1)
    plane = lax.axis_index(ZH).astype(jnp.int32).reshape(1)

    packed = pack(samples, where, plane, planes, members, quarters)
    quarter = lax.all_to_all(packed, PLANE, split_axis=0, concat_axis=0, tiled=True)
    from_below = shifted(weight, ZH, 1)
    from_above = shifted(weight, ZH, -1)
    far_head = shifted(from_below[:depth // 2], ZH, 1)
    far_rest = shifted(from_above[depth // 2:], ZH, -1)
    near = {"0": weight, "1": from_below, "2_head": far_head, "2_rest": far_rest, "3": from_above}
    pairs = []
    for piece in near.values():
        other = shifted(piece, ZL, 1)
        pairs.append(jnp.concatenate([piece, other], axis=1))
    by_pair = jnp.concatenate(pairs, axis=0)
    by_all = jnp.concatenate([by_pair, shifted(by_pair, CORE, 1)], axis=1)
    middle = samples.shape[1] * 3 // 4
    gram_head = self_product(samples[:, :middle])

    flat = quarter.reshape(members * part, planes * depth)
    early = members * EARLY // 16 * part
    beside_a = shifted(flat[:early], ZL, 1)
    partial = jnp.dot(flat, by_all, preferred_element_type=F32)
    partial, late = lax.optimization_barrier((partial, flat))
    partial = lax.all_to_all(partial.reshape(members, part, quarters * width), PLANE, split_axis=0, concat_axis=0, tiled=True)
    across = shifted(flat, CORE, 1)
    diagonal_a = shifted(beside_a, CORE, 1)
    gram_rest = lax.optimization_barrier(self_product(samples[:, middle:]))
    gram = gram_head + gram_rest
    ready = prepare(gram, inverse, width)
    partial, late = lax.optimization_barrier((partial, late[early:]))
    own_piece, by_core, by_line, by_both = gathered(partial)
    by_line = shifted(by_line, ZL, 1)
    by_both = lax.ppermute(by_both, CLS, [(i, i ^ 3) for i in range(4)])
    by_core = shifted(by_core, CORE, 1)
    start = [own_piece, by_core, by_line, by_both]
    beside_b = shifted(late, ZL, 1)

    alpha, steps, top = passes(where, start, labels[None, :], dual, ready, members)
    steps = lax.all_to_all(steps, PLANE, split_axis=0, concat_axis=0, tiled=True)
    diagonal_b = shifted(beside_b, CORE, 1)

    top = top[0]
    other = shifted(top, CORE, 1)
    top = jnp.maximum(top, other)
    other = shifted(top, ZL, 1)
    top = jnp.maximum(top, other)

    held = [flat, across, beside_a, beside_b, diagonal_a, diagonal_b]
    far = planes // 2
    sent, turned, gap = first_delta(where, held, steps, planes, far)
    came = [shifted(sent, ZH, planes - far)]
    for k in reversed(range(1, planes)):
        if k != far:
            sent = next_delta(held, turned, gap, planes, k)
            came.append(shifted(sent, ZH, planes - k))
    own = own_delta(held, turned, planes)
    new_weight, gap = finish(weight, own, gap, came, rows * planes * members)
    return new_weight, alpha, gap[0], top


def solution(mesh):
    fine = Mesh(mesh.devices.reshape(4, 4, 4, 2, 2), (ZH, X, Y, ZL, CORE))
    return jax.shard_map(
        round_of_ascent,
        mesh=fine,
        in_specs=(P(SAMP, None), P(SAMP), P(SAMP, CLS), P(SAMP, CLS), P(SAMP, None, None)),
        out_specs=(P(SAMP, CLS), P(SAMP, CLS), P(CLS), P(SAMP)),
        check_vma=False,
    )
```
